32 devices in a mesh: ctx: 8 (over z, y), head: 4 (over x, core).
Axes of the slice: x: 2, y: 2, z: 4, core: 2. Of those that a mesh axis runs over, the one named last changes fastest.
Arguments:
- patches: bfloat16 [4096, 1152], P(('ctx', 'head')), may hold values from -44 to 44
- clip_start: int32 [8], replicated, may hold values from 0 to 511, as said below
- clip_len: int32 [8], replicated, may hold values from 1 to 512
- text_rows: bfloat16 [4096, 2048], P('ctx', 'head'), may hold values from -6 to 6
- vision_qkv: bfloat16 [1152, 3, 1152], P(None, None, 'head'), may hold values from -10 to 10
- vision_out: bfloat16 [1152, 1152], P('head'), may hold values from -0.75 to 0.75
- projector: bfloat16 [1152, 2048], P(None, 'head'), may hold values from -0.1875 to 0.1875
- layer_qkv: bfloat16 [2048, 3, 2048], P(None, None, 'head'), may hold values from -0.125 to 0.125
- head_gain: float32 [2048], P('head'), may hold values from 0.5 to 1.5
- state_in: float32 [16, 128, 128], P('head'), may hold values from -32768 to 32768
Outputs:
- attended: bfloat16 [4096, 2048], P('ctx', 'head')
The draws below stay inside these ranges and needn't reach their ends.
Inputs may be any that keep to these rules, and one draw needn't show every extreme that they name: Clip c occupies clip_len[c] positions from c * 512 + clip_start[c] on; no two clips share a position, and the last clip ends within the last 512 positions.
All inputs are finite; a program needn't handle non-finite values.
Results may differ from the reference program's by a relative error of at most 0.015.
Values may be sent and summed in bfloat16 or wider, within the bound.
No kernel may reach another device: no remote copies, remote signals or barrier semaphores. Data moves between devices by JAX's collectives and lax.ppermute only.
A program may use at most 64 MiB of HBM per device.

```python
import math
import jax
import jax.numpy as jnp
from jax import lax

D_VIT = 1152
VIT_HEADS = 16
VIT_HD = 72
D = 2048
HEADS = 16
HD = 128
TOK_CTX = 512
NCLIP = 8
SEQ = 4096
PRIOR = 2048


def clip_layout(key):
    gap_key, size_key, pick_key = jax.random.split(jax.random.fold_in(key, 11), 3)
    gaps = jax.random.randint(gap_key, (NCLIP,), 0, TOK_CTX // 2 + 1)
    sizes = jax.random.randint(size_key, (NCLIP,), TOK_CTX // 4, TOK_CTX + 1)
    chosen = jax.random.randint(pick_key, (), 0, NCLIP - 1)
    sizes = jnp.where(jnp.arange(NCLIP) == chosen, TOK_CTX, sizes)
    before_last = jnp.arange(NCLIP) == NCLIP - 2
    gaps = jnp.where(before_last, jnp.maximum(gaps, TOK_CTX // 4), gaps)
    sizes = jnp.where(before_last, TOK_CTX, sizes)

    def advance(floor, item):
        gap, size, index = item
        start = jnp.minimum(floor + gap, TOK_CTX - 1)
        start = jnp.where(index == NCLIP - 1, TOK_CTX - 1, start)
        size = jnp.where(index == NCLIP - 1, jnp.minimum(size, TOK_CTX - start), size)
        size = jnp.maximum(size, 1)
        return (jnp.maximum(start + size - TOK_CTX, 0), (start, size))
    _, (starts, lengths) = lax.scan(advance, jnp.zeros((), jnp.int32), (gaps, sizes, jnp.arange(NCLIP)))
    return (starts.astype(jnp.int32), lengths.astype(jnp.int32))


def draw_clip_start(key, part):
    return clip_layout(key)[0]


def draw_clip_len(key, part):
    return clip_layout(key)[1]


def draw_patches(key, part):
    base_key = jax.random.fold_in(jax.random.fold_in(key, 21), 0)
    values = jax.random.truncated_normal(base_key, -4.0, 4.0, (NCLIP, TOK_CTX, D_VIT), jnp.float32)
    return values.reshape(NCLIP * TOK_CTX, D_VIT).astype(jnp.bfloat16)


def draw_vision_qkv(key, part):
    parts = jax.random.split(jax.random.fold_in(key, 31), 3)
    shape = (D_VIT, VIT_HEADS, VIT_HD)
    factor = D_VIT ** (-0.5)
    query = jax.random.truncated_normal(parts[0], -4.0, 4.0, shape, jnp.float32) * factor
    keys = jax.random.truncated_normal(parts[1], -4.0, 4.0, shape, jnp.float32) * factor
    values = jax.random.truncated_normal(parts[2], -4.0, 4.0, shape, jnp.float32) * factor
    whole = jnp.stack([query, keys, values], axis=1).reshape(D_VIT, 3, D_VIT)
    return jnp.clip(whole, -10.0, 10.0).astype(jnp.bfloat16)


def draw_state_in(key, part):
    key_part, value_part = jax.random.split(jax.random.fold_in(key, 41), 2)
    earlier_keys = jax.random.truncated_normal(key_part, -4.0, 4.0, (PRIOR, HEADS, HD), jnp.float32)
    earlier_values = jax.random.truncated_normal(value_part, -4.0, 4.0, (PRIOR, HEADS, HD), jnp.float32)
    return jnp.einsum('shd,she->hde', earlier_keys, earlier_values).astype(jnp.float32)


def block_levels(rng, shape, cuts, least, high):
    gain, own = 1.0, jax.random.fold_in(rng, 6)
    for dim, blocks in cuts:
        heights = jnp.exp(jax.random.uniform(jax.random.fold_in(own, dim), (blocks,), jnp.float32, least / len(cuts), high / len(cuts)))
        gain = gain * jnp.repeat(heights, shape[dim] // blocks).reshape([-1 if axis == dim else 1 for axis in range(len(shape))])
    return gain


def bell_draw(own_key, extent, spread, reach, cuts=(), kind=jnp.bfloat16):
    values = jax.random.normal(own_key, extent, jnp.float32) * spread
    if len(cuts) > 0:
        values = block_levels(own_key, extent, cuts, -0.22, 0.18) * values
    return jnp.clip(values, min=-reach, max=reach).astype(kind)


def setup_inputs(seed: int = 0) -> dict:
    streams_of = jax.random.split(jax.random.key(seed), 11)
    return {
        "patches": draw_patches(jax.random.fold_in(streams_of[10], 71), 0),
        "clip_start": draw_clip_start(jax.random.fold_in(streams_of[10], 71), 0),
        "clip_len": draw_clip_len(jax.random.fold_in(streams_of[10], 71), 0),
        "text_rows": bell_draw(streams_of[3], (SEQ, D), 1.0, 6.0, ((0, 8), (1, 4))),
        "vision_qkv": draw_vision_qkv(jax.random.fold_in(streams_of[10], 71), 0),
        "vision_out": bell_draw(streams_of[5], (D_VIT, D_VIT), VIT_HD ** -0.5, 0.75, ((0, 4),)),
        "projector": bell_draw(streams_of[6], (D_VIT, D), D_VIT ** -0.5, 0.1875, ((1, 4),)),
        "layer_qkv": bell_draw(streams_of[7], (D, 3, D), D ** -0.5, 0.125, ((2, 4),)),
        "head_gain": jnp.clip(1.0 + 0.1 * jax.random.normal(streams_of[8], (D,), jnp.float32), 0.5, 1.5),
        "state_in": draw_state_in(jax.random.fold_in(streams_of[10], 71), 0),
    }


EPS = 1e-06
HIGH = lax.Precision.HIGHEST

def unit_rows(values):
    values = values.astype(jnp.float32)
    return values * lax.rsqrt(lax.optimization_barrier(jnp.mean(values * values, axis=-1, keepdims=True)) + EPS)

def encode_clip(frame, length, vision_qkv, vision_out, projector):
    rows = frame.shape[0]
    normed = unit_rows(frame).astype(jnp.bfloat16)
    mixed = jnp.dot(normed, vision_qkv.reshape(D_VIT, 3 * D_VIT), preferred_element_type=jnp.float32).astype(jnp.bfloat16)
    mixed = mixed.reshape(rows, 3, VIT_HEADS, VIT_HD).astype(jnp.float32)
    scores = jnp.einsum('thd,shd->hts', mixed[:, 0], mixed[:, 1]) * VIT_HD ** (-0.5)
    live = jnp.arange(rows) < length
    scores = jnp.where(live[None, None, :], scores, -jnp.inf)
    highest = lax.optimization_barrier(jnp.max(scores, axis=-1, keepdims=True))
    powers = jnp.exp(scores - highest)
    probs = (powers / lax.optimization_barrier(jnp.sum(powers, axis=-1, keepdims=True))).astype(jnp.bfloat16)
    context = jnp.einsum('hts,shd->thd', probs.astype(jnp.float32), mixed[:, 2])
    context = context.astype(jnp.bfloat16).reshape(rows, D_VIT)
    resid = frame.astype(jnp.float32) + jnp.dot(context, vision_out, preferred_element_type=jnp.float32)
    merged = unit_rows(resid).astype(jnp.bfloat16)
    return jnp.dot(merged, projector, preferred_element_type=jnp.float32).astype(jnp.bfloat16)

def reference(patches, clip_start, clip_len, text_rows, vision_qkv, vision_out, projector, layer_qkv, head_gain, state_in):
    frames = patches.reshape(NCLIP, TOK_CTX, D_VIT)

    def encode(item):
        return encode_clip(item[0], item[1], vision_qkv, vision_out, projector)
    visual = lax.map(encode, (frames, clip_len)).reshape(SEQ, D)
    position = jnp.arange(SEQ).astype(jnp.int32)
    owner = position // TOK_CTX
    within = position % TOK_CTX
    offset = within - clip_start[owner]
    own_live = (offset >= 0) & (offset < clip_len[owner])
    prior = jnp.maximum(owner - 1, 0)
    later = within + TOK_CTX - clip_start[prior]
    prior_live = (owner > 0) & (later < clip_len[prior])
    own_rows = visual[(owner * TOK_CTX + jnp.clip(offset, 0, TOK_CTX - 1)).astype(jnp.int32)]
    prior_rows = visual[(prior * TOK_CTX + jnp.clip(later, 0, TOK_CTX - 1)).astype(jnp.int32)]
    sequence = jnp.where(own_live[:, None], own_rows, jnp.where(prior_live[:, None], prior_rows, text_rows))
    unit = unit_rows(sequence).astype(jnp.bfloat16)
    layer_mix = jnp.dot(unit, layer_qkv.reshape(D, 3 * D), preferred_element_type=jnp.float32).astype(jnp.bfloat16)
    layer_mix = layer_mix.reshape(SEQ, 3, HEADS, HD)
    block = math.gcd(SEQ, 512)
    count = SEQ // block
    pieces = layer_mix.reshape(count, block, 3, HEADS, HD)
    causal = jnp.arange(block)[:, None] >= jnp.arange(block)[None, :]

    def advance(state, piece):
        piece = piece.astype(jnp.float32)
        query, keys, values = (piece[:, 0], piece[:, 1], piece[:, 2])
        inter = jnp.einsum('thd,hde->the', query, state, precision=HIGH)
        weights = jnp.einsum('thd,shd->hts', query, keys, precision=HIGH)
        weights = jnp.where(causal[None], weights, 0.0)
        intra = jnp.einsum('hts,she->the', weights, values, precision=HIGH)
        state = state + jnp.einsum('shd,she->hde', keys, values, precision=HIGH)
        return (state, inter + intra)
    start_state = state_in.astype(jnp.float32)
    _, lin = lax.scan(advance, start_state, pieces)
    lin = lin.reshape(SEQ, HEADS, HD)
    scaled = lin * lax.rsqrt(lax.optimization_barrier(jnp.mean(lin * lin, axis=-1, keepdims=True)) + EPS)
    scaled = scaled * head_gain.reshape(HEADS, HD).astype(jnp.float32)
    return scaled.astype(jnp.bfloat16).reshape(SEQ, D)
```

```python
import jax
import jax.numpy as jnp
from jax import lax
from jax.sharding import PartitionSpec as P

VIT_HEADS = 16
VIT_HD = 72
HEADS = 16
HD = 128


EPS = 1e-06


def shifted(value, axis, steps):
    count = lax.axis_size(axis)
    return lax.ppermute(value, axis, [(source, source + steps) for source in range(count - steps)])


def swapped(value, axis, bit):
    count = lax.axis_size(axis)
    return lax.ppermute(value, axis, [(source, source ^ bit) for source in range(count)])


def gathered(value, axis):
    count = lax.axis_size(axis)
    blocks = [value] + [None] * (count - 1)
    far = count // 2
    stride = far
    known = [0]
    while stride >= 1:
        fresh = []
        for key in known:
            blocks[key ^ stride] = swapped(blocks[key], axis, stride)
            fresh.append(key ^ stride)
        known = known + fresh
        stride //= 2
    return blocks


def in_order(blocks, axis):
    place = lax.axis_index(axis)
    count = len(blocks)
    stack = list(blocks)
    stride = 1
    while stride < count:
        flip = (place & stride) != 0
        stack = [jnp.where(flip, stack[key ^ stride], stack[key]) for key in range(count)]
        stride *= 2
    return stack


def earlier_sum(value, axis):
    count = lax.axis_size(axis)
    place = lax.axis_index(axis)
    wide = lambda part: part.astype(jnp.float32)
    slim = lambda part: part.astype(jnp.bfloat16)
    partner = swapped(value, axis, 1)
    total = wide(value) + wide(partner)
    before = jnp.where(place % 2 == 1, wide(partner), 0.0)
    pairs = jnp.zeros_like(total)
    step = 1
    while 2 * step < count:
        arrived = wide(shifted(slim(total), axis, 2 * step))
        pairs = pairs + arrived
        total = total + arrived
        step *= 2
    return before + pairs


def unit_rows(values):
    values = values.astype(jnp.float32)
    return values * lax.rsqrt(jnp.mean(values * values, axis=-1, keepdims=True) + EPS)


def clip_attention(frame, length, vision_qkv, head_count):
    rows = frame.shape[0]
    normed = unit_rows(frame).astype(jnp.bfloat16)
    mixed = jnp.dot(
        normed, vision_qkv.reshape(vision_qkv.shape[0], -1), preferred_element_type=jnp.float32
    )
    mixed = mixed.astype(jnp.bfloat16).reshape(rows, 3, head_count, VIT_HD)
    scores = jnp.einsum(
        "thd,shd->hts", mixed[:, 0], mixed[:, 1], preferred_element_type=jnp.float32
    ) * VIT_HD ** (-0.5)
    live = jnp.arange(rows) < length
    scores = jnp.where(live[None, None, :], scores, -jnp.inf)
    highest = jnp.max(scores, axis=-1, keepdims=True)
    powers = jnp.exp(scores - highest)
    probs = (powers / jnp.sum(powers, axis=-1, keepdims=True)).astype(jnp.bfloat16)
    context = jnp.einsum("hts,shd->thd", probs, mixed[:, 2], preferred_element_type=jnp.float32)
    return context.astype(jnp.bfloat16).reshape(rows, head_count * VIT_HD)


def local(
    patches,
    clip_start,
    clip_len,
    text_rows,
    vision_qkv,
    vision_out,
    projector,
    layer_qkv,
    head_gain,
    state_in,
):
    groups = lax.axis_size("head")
    place = lax.axis_index("ctx")
    span = text_rows.shape[0]
    length = lax.dynamic_index_in_dim(clip_len, place, keepdims=False)
    start = lax.dynamic_index_in_dim(clip_start, place, keepdims=False)
    frame = jnp.concatenate(in_order(gathered(patches, "head"), "head"), axis=0)
    outs = gathered(vision_out, "head")
    context = clip_attention(frame, length, vision_qkv, VIT_HEADS // groups)
    contexts = gathered(context, "head")
    total = frame.astype(jnp.float32)
    total = total + jnp.dot(
        jnp.concatenate(contexts, axis=1),
        jnp.concatenate(outs, axis=0),
        preferred_element_type=jnp.float32,
    )
    merged = unit_rows(total).astype(jnp.bfloat16)
    visual = jnp.dot(merged, projector, preferred_element_type=jnp.float32).astype(jnp.bfloat16)
    within = jnp.arange(span)
    visual = jnp.where((within < length)[:, None], visual, jnp.zeros_like(visual))
    window = jnp.zeros((2 * span, visual.shape[1]), jnp.bfloat16)
    window = lax.dynamic_update_slice_in_dim(window, visual, start, 0)
    arrived = shifted(window[span:], "ctx", 1)
    own_live = (within >= start) & (within < start + length)
    prior = jnp.maximum(place - 1, 0)
    prior_start = lax.dynamic_index_in_dim(clip_start, prior, keepdims=False)
    prior_len = lax.dynamic_index_in_dim(clip_len, prior, keepdims=False)
    prior_live = (place > 0) & (within + span - prior_start < prior_len)
    sequence = jnp.where(
        own_live[:, None], window[:span], jnp.where(prior_live[:, None], arrived, text_rows)
    )
    full = jnp.concatenate(in_order(gathered(sequence, "head"), "head"), axis=1)
    unit = unit_rows(full).astype(jnp.bfloat16)
    heads = HEADS // groups
    layer_mix = jnp.dot(
        unit, layer_qkv.reshape(layer_qkv.shape[0], -1), preferred_element_type=jnp.float32
    )
    layer_mix = layer_mix.astype(jnp.bfloat16).reshape(span, 3, heads, HD)
    query, keys, values = (layer_mix[:, 0], layer_mix[:, 1], layer_mix[:, 2])
    delta = jnp.einsum("shd,she->hde", keys, values, preferred_element_type=jnp.float32)
    carried = earlier_sum(delta.astype(jnp.bfloat16), "ctx") + state_in
    weights = jnp.einsum("thd,shd->hts", query, keys, preferred_element_type=jnp.float32)
    causal = within[:, None] >= within[None, :]
    weights = jnp.where(causal[None], weights, 0.0).astype(jnp.bfloat16)
    intra = jnp.einsum("hts,she->the", weights, values, preferred_element_type=jnp.float32)
    inter = jnp.einsum(
        "thd,hde->the", query, carried.astype(jnp.bfloat16), preferred_element_type=jnp.float32
    )
    lin = inter + intra
    scaled = lin * lax.rsqrt(jnp.mean(lin * lin, axis=-1, keepdims=True) + EPS)
    scaled = scaled * head_gain.reshape(heads, HD)
    return scaled.astype(jnp.bfloat16).reshape(span, heads * HD)


def solution(mesh):
    placed = (
        P(("ctx", "head"), None),
        P(),
        P(),
        P("ctx", "head"),
        P(None, None, "head"),
        P("head", None),
        P(None, "head"),
        P(None, None, "head"),
        P("head"),
        P("head", None, None),
    )
    return jax.shard_map(
        local, mesh=mesh, in_specs=placed, out_specs=P("ctx", "head"), check_vma=False
    )
```

```python
import functools
import math

import jax
import jax.numpy as jnp
from jax import lax
from jax.experimental import pallas as pl
from jax.experimental.pallas import tpu as pltpu
from jax.sharding import PartitionSpec as P

VIT_HEADS = 16
VIT_HD = 72
HEADS = 16
HD = 128

EPS = 1e-06
LOW = -1e30
BLOCK = 128
VMEM = pl.BlockSpec(memory_space=pltpu.VMEM)
SMEM = pl.BlockSpec(memory_space=pltpu.SMEM)
F32 = jnp.float32
BF16 = jnp.bfloat16


def dot(left, right):
    return jnp.dot(left, right, preferred_element_type=F32)


def dot_t(left, right):
    return lax.dot_general(left, right, (((1,), (1,)), ((), ())), preferred_element_type=F32)


def shifted(value, axis, steps):
    count = lax.axis_size(axis)
    return lax.ppermute(value, axis, [(source, source + steps) for source in range(count - steps)])


def swapped(value, axis, bit):
    count = lax.axis_size(axis)
    return lax.ppermute(value, axis, [(source, source ^ bit) for source in range(count)])


def spread(value, axis):
    count = lax.axis_size(axis)
    blocks = {0: value}
    stride = count // 2
    while stride >= 1:
        for key in list(blocks):
            blocks[key ^ stride] = swapped(blocks[key], axis, stride)
        stride //= 2
    return [blocks[key] for key in range(count)]


def spread_prior(value):
    count = lax.axis_size("head")
    groups = lax.axis_size("ctx")
    stride = count // 2
    blocks = {0: shifted(value, "ctx", 1)}
    pairs = [
        (group * count + member, (group + 1) * count + (member ^ stride))
        for group in range(groups - 1)
        for member in range(count)
    ]
    blocks[stride] = lax.ppermute(value, ("ctx", "head"), pairs)
    stride //= 2
    while stride >= 1:
        for key in list(blocks):
            blocks[key ^ stride] = swapped(blocks[key], "head", stride)
        stride //= 2
    return [blocks[key] for key in range(count)]


def earlier_sum(value, axis):
    count = lax.axis_size(axis)
    place = lax.axis_index(axis)
    partner = swapped(value, axis, 1)
    total = value.astype(F32) + partner.astype(F32)
    before = jnp.where(place % 2 == 1, partner.astype(F32), 0.0)
    parts = [before]
    step = 1
    while 2 * step < count:
        arrived = shifted(total.astype(BF16), axis, 2 * step).astype(F32)
        parts.append(arrived)
        total = total + arrived
        step *= 2
    return sum(parts)


def clip_span(starts, lens, span, prior):
    place = lax.axis_index("ctx")
    if prior:
        source = jnp.maximum(place - 1, 0)
        shift = span - starts[source]
        length = jnp.where(place > 0, lens[source], 0)
    else:
        shift = -starts[place]
        length = lens[place]
    return shift, length, jnp.maximum(0, -shift), jnp.minimum(span, length - shift)


def clip_rows(rows, count, span):
    me = lax.axis_index("head")
    slot = lax.broadcasted_iota(jnp.int32, (1, span), 1)
    row = slot
    for key in range(count):
        inside = (slot >= key * rows) & (slot < (key + 1) * rows)
        row = jnp.where(inside, slot + ((me ^ key) - key) * rows, row)
    return row


def attend_kernel(prior, heads, block, starts, lens, *refs):
    count = len(refs) - (6 if prior else 5)
    pieces = refs[:count]
    weights, *olds, context, queries, keys, values = refs[count:]
    rows, width = pieces[0].shape
    span = rows * count
    inner = weights.shape[0] // 3
    size = inner // heads
    shift, length, first, last = clip_span(starts, lens, span, prior)
    context[...] = olds[0][...] if prior else jnp.zeros_like(context)
    row = clip_rows(rows, count, span)
    lane = lax.broadcasted_iota(jnp.int32, (1, inner), 1)
    owner = [(lane >= head * size) & (lane < (head + 1) * size) for head in range(heads)]
    groups = {}
    for head in range(heads):
        groups.setdefault(head * size // 128 * 128, []).append(head)

    @pl.when(last > first)
    def _():
        frame = jnp.concatenate([piece[...] for piece in pieces], axis=0)
        wide = frame.astype(F32)
        scale = lax.rsqrt(jnp.sum(wide * wide, axis=-1, keepdims=True) * (1.0 / width) + EPS)
        full = dot_t(frame, weights[...])
        queries[...] = (full[:, :inner] * (scale * (size**-0.5 * math.log2(math.e)))).astype(BF16)
        keys[...] = (full[:, inner : 2 * inner] * scale).astype(BF16)
        values[...] = (full[:, 2 * inner :] * scale).astype(BF16)

    def step(index, _):
        low = pl.multiple_of(index * block, block)
        place = low + lax.broadcasted_iota(jnp.int32, (block, 1), 0)
        live = (place >= first) & (place < last)
        pick = (place + shift == row) & live
        query = dot(jnp.where(pick, 1.0, 0.0).astype(BF16), queries[...])
        total = jnp.zeros((block, inner), F32)
        for base, members in groups.items():
            end = min(inner, base + 256)
            stack = jnp.concatenate(
                [jnp.where(owner[head], query, 0.0)[:, base:end].astype(BF16) for head in members], axis=0
            )
            scores = dot_t(stack, keys[:, base:end])
            scores = jnp.where(row < length, scores, LOW)
            powers = jnp.exp2(scores - jnp.max(scores, axis=-1, keepdims=True))
            mass = jnp.sum(powers, axis=-1, keepdims=True)
            mixed = dot(powers.astype(BF16), values[:, base:end]) / mass
            for place_in, head in enumerate(members):
                part = mixed[place_in * block : (place_in + 1) * block, :]
                sides = [part]
                if base:
                    sides = [jnp.zeros((block, base), F32)] + sides
                if end < inner:
                    sides = sides + [jnp.zeros((block, inner - end), F32)]
                total = jnp.where(owner[head], jnp.concatenate(sides, axis=1), total)
        here = pl.ds(low, block)
        if prior:
            context[here, :] = jnp.where(live, total, context[here, :].astype(F32)).astype(BF16)
        else:
            context[here, :] = total.astype(BF16)
        return 0

    lax.fori_loop(first // block, jnp.where(last > first, (last + block - 1) // block, 0), step, 0)


def attend(pieces, weights, starts, lens, heads, old=None):
    rows, width = pieces[0].shape
    span = rows * len(pieces)
    inner = weights.shape[0] // 3
    olds = [] if old is None else [old]
    return pl.pallas_call(
        functools.partial(attend_kernel, old is not None, heads, min(BLOCK, span)),
        out_shape=jax.ShapeDtypeStruct((span, inner), BF16),
        in_specs=[SMEM, SMEM] + [VMEM] * (len(pieces) + 1 + len(olds)),
        out_specs=VMEM,
        scratch_shapes=[pltpu.VMEM((span, inner), BF16)] * 3,
        compiler_params=pltpu.CompilerParams(vmem_limit_bytes=16 * 2**20),
        cost_estimate=pl.CostEstimate(flops=5 * 10**9, bytes_accessed=4 * 10**6, transcendentals=10**6),
        name="attend_prior" if olds else "attend_own",
    )(starts, lens, *pieces, weights, *olds)


def arrange_kernel(starts, lens, *refs):
    frame_out = refs[-1]
    count = (len(refs) - 1) // 2
    rows, width = refs[0].shape
    span = rows * count
    row = clip_rows(rows, count, span)
    place = lax.broadcasted_iota(jnp.int32, (span, 1), 0)
    total = 0.0
    for prior in (False, True):
        shift, length, _, _ = clip_span(starts, lens, span, prior)
        pick = (place + shift == row) & (row < length)
        frame = jnp.concatenate([piece[...] for piece in refs[prior * count : (prior + 1) * count]], axis=0)
        total = total + dot(jnp.where(pick, 1.0, 0.0).astype(BF16), frame)
    frame_out[...] = total.astype(BF16)


def arrange(own, prior, starts, lens):
    rows, width = own[0].shape
    span = rows * len(own)
    return pl.pallas_call(
        arrange_kernel,
        out_shape=jax.ShapeDtypeStruct((span, width), BF16),
        in_specs=[SMEM, SMEM] + [VMEM] * (2 * len(own)),
        out_specs=VMEM,
        compiler_params=pltpu.CompilerParams(vmem_limit_bytes=12 * 2**20),
        cost_estimate=pl.CostEstimate(flops=2 * 10**9, bytes_accessed=3 * 10**6, transcendentals=0),
        name="arrange",
    )(starts, lens, *own, *prior)


def project_kernel(starts, lens, *refs):
    count = (len(refs) - 4) // 2
    frame, projector, text, *pieces, result = refs
    parts, weights = pieces[:count], pieces[count:]
    span = frame.shape[0]
    _, _, own_first, own_last = clip_span(starts, lens, span, False)
    _, _, prior_first, prior_last = clip_span(starts, lens, span, True)
    context = jnp.concatenate([part[...] for part in parts], axis=1)
    out_weight = jnp.concatenate([weight[...] for weight in weights], axis=0)
    resid = frame[...].astype(F32) + dot(context, out_weight)
    scale = lax.rsqrt(jnp.mean(resid * resid, axis=-1, keepdims=True) + EPS)
    visual = dot((resid * scale).astype(BF16), projector[...]).astype(BF16)
    place = lax.broadcasted_iota(jnp.int32, (span, 1), 0)
    live = ((place >= own_first) & (place < own_last)) | (
        (place >= prior_first) & (place < prior_last)
    )
    result[...] = jnp.where(live, visual, text[...])


def project(frame, parts, outs, projector, text, starts, lens):
    return pl.pallas_call(
        project_kernel,
        out_shape=jax.ShapeDtypeStruct(text.shape, BF16),
        in_specs=[SMEM, SMEM] + [VMEM] * (3 + 2 * len(parts)),
        out_specs=VMEM,
        compiler_params=pltpu.CompilerParams(vmem_limit_bytes=14 * 2**20),
        cost_estimate=pl.CostEstimate(flops=3 * 10**9, bytes_accessed=4 * 10**6, transcendentals=0),
        name="project",
    )(starts, lens, frame, projector, text, *parts, *outs)


def held(weights, part, key, depth):
    start = pl.multiple_of((lax.axis_index("head") ^ key) * depth, depth)
    return weights[part, pl.ds(start, depth), :]


def near_kernel(keys, weights, *refs):
    count = len(keys)
    pieces = refs[:count]
    query_sum, pair_sum, squares = refs[count:]
    norm = 0.0
    for piece in pieces:
        wide = piece[...].astype(F32)
        norm = norm + jnp.sum(wide * wide, axis=-1, keepdims=True)
    squares[...] = jnp.broadcast_to(norm, squares.shape)
    for part in range(3):
        total = 0.0
        for index in range(count):
            total = total + dot(pieces[index][...], held(weights, part, keys[index], pieces[index].shape[1]))
        if part == 0:
            query_sum[...] = total
        else:
            pair_sum[part - 1] = total


def near(pieces, keys, weights):
    span, depth = pieces[0].shape
    columns = weights.shape[2]
    return pl.pallas_call(
        functools.partial(near_kernel, keys),
        out_shape=(
            jax.ShapeDtypeStruct((span, columns), F32),
            jax.ShapeDtypeStruct((2, span, columns), F32),
            jax.ShapeDtypeStruct((span, HD), F32),
        ),
        in_specs=[VMEM] * (1 + len(pieces)),
        out_specs=(VMEM, VMEM, VMEM),
        compiler_params=pltpu.CompilerParams(vmem_limit_bytes=12 * 2**20),
        cost_estimate=pl.CostEstimate(flops=3 * 10**9, bytes_accessed=7 * 10**6, transcendentals=0),
        name="near",
    )(weights, *pieces)


def pair_kernel(keys, total_depth, weights, pair_sum, squares, *refs):
    count = len(keys)
    pieces = refs[:count]
    key_out, value_out, delta, scale_out = refs[count:]
    norm = squares[:, :1]
    for piece in pieces:
        wide = piece[...].astype(F32)
        norm = norm + jnp.sum(wide * wide, axis=-1, keepdims=True)
    scale = lax.rsqrt(norm * (1.0 / total_depth) + EPS)
    scale_out[...] = jnp.broadcast_to(scale, scale_out.shape)
    for part, out in ((0, key_out), (1, value_out)):
        total = pair_sum[part]
        for index in range(count):
            total = total + dot(pieces[index][...], held(weights, part + 1, keys[index], pieces[index].shape[1]))
        out[...] = (total * scale).astype(BF16)
    for head in range(delta.shape[0]):
        lanes = slice(head * HD, (head + 1) * HD)
        delta[head] = lax.dot_general(
            key_out[:, lanes], value_out[:, lanes], (((0,), (0,)), ((), ())), preferred_element_type=F32
        ).astype(BF16)


def pair(pieces, keys, weights, pair_sum, squares):
    span, depth = pieces[0].shape
    columns = weights.shape[2]
    return pl.pallas_call(
        functools.partial(pair_kernel, keys, weights.shape[1]),
        out_shape=(
            jax.ShapeDtypeStruct((span, columns), BF16),
            jax.ShapeDtypeStruct((span, columns), BF16),
            jax.ShapeDtypeStruct((columns // HD, HD, HD), BF16),
            jax.ShapeDtypeStruct((span, HD), F32),
        ),
        in_specs=[VMEM] * (3 + len(pieces)),
        out_specs=(VMEM,) * 4,
        compiler_params=pltpu.CompilerParams(vmem_limit_bytes=12 * 2**20),
        cost_estimate=pl.CostEstimate(flops=3 * 10**9, bytes_accessed=7 * 10**6, transcendentals=0),
        name="pair",
    )(weights, pair_sum, squares, *pieces)


def within_kernel(keys, weights, query_sum, scale, key_in, value_in, *refs):
    count = len(keys)
    pieces = refs[:count]
    query_out, intra = refs[count:]
    span = query_sum.shape[0]
    total = query_sum[...]
    for index in range(count):
        total = total + dot(pieces[index][...], held(weights, 0, keys[index], pieces[index].shape[1]))
    query_out[...] = (total * scale[:, :1]).astype(BF16)
    half = span // 2
    causal = lax.broadcasted_iota(jnp.int32, (half, half), 0) >= lax.broadcasted_iota(
        jnp.int32, (half, half), 1
    )
    for head in range(query_out.shape[1] // HD):
        lanes = slice(head * HD, (head + 1) * HD)
        for top in (0, half):
            query = query_out[top : top + half, lanes]
            corner = dot_t(query, key_in[top : top + half, lanes])
            corner = jnp.where(causal, corner, 0.0).astype(BF16)
            piece = dot(corner, value_in[top : top + half, lanes])
            if top:
                left = dot_t(query, key_in[:top, lanes]).astype(BF16)
                piece = piece + dot(left, value_in[:top, lanes])
            intra[top : top + half, lanes] = piece


def within(pieces, keys, weights, query_sum, scale, key_in, value_in):
    span, depth = pieces[0].shape
    columns = weights.shape[2]
    return pl.pallas_call(
        functools.partial(within_kernel, keys),
        out_shape=(
            jax.ShapeDtypeStruct((span, columns), BF16),
            jax.ShapeDtypeStruct((span, columns), F32),
        ),
        in_specs=[VMEM] * (5 + len(pieces)),
        out_specs=(VMEM,) * 2,
        compiler_params=pltpu.CompilerParams(vmem_limit_bytes=12 * 2**20),
        cost_estimate=pl.CostEstimate(flops=3 * 10**9, bytes_accessed=5 * 10**6, transcendentals=0),
        name="within",
    )(weights, query_sum, scale, key_in, value_in, *pieces)


def finish_kernel(query, intra, carried, state, gain, out):
    for head in range(state.shape[0]):
        lanes = slice(head * HD, (head + 1) * HD)
        whole = (carried[head] + state[head]).astype(BF16)
        lin = intra[:, lanes] + dot(query[:, lanes], whole)
        scale = lax.rsqrt(jnp.mean(lin * lin, axis=-1, keepdims=True) + EPS)
        out[:, lanes] = (lin * scale * gain[:, lanes]).astype(BF16)


def finish(query, intra, carried, state, gain):
    return pl.pallas_call(
        finish_kernel,
        out_shape=jax.ShapeDtypeStruct(query.shape, BF16),
        in_specs=[VMEM] * 5,
        out_specs=VMEM,
        compiler_params=pltpu.CompilerParams(vmem_limit_bytes=8 * 2**20),
        cost_estimate=pl.CostEstimate(flops=10**8, bytes_accessed=3 * 10**6, transcendentals=0),
        name="finish",
    )(query, intra, carried, state, gain.reshape(1, -1))


def local(
    patches,
    clip_start,
    clip_len,
    text_rows,
    vision_qkv,
    vision_out,
    projector,
    layer_qkv,
    head_gain,
    state_in,
):
    groups = lax.axis_size("head")
    heads = VIT_HEADS // groups
    own = spread(patches, "head")
    prior = spread_prior(patches)
    outs = spread(vision_out, "head")
    vision = jnp.transpose(vision_qkv, (1, 2, 0)).reshape(-1, vision_qkv.shape[0])
    layer = jnp.transpose(layer_qkv, (1, 0, 2))
    context = attend(own, vision, clip_start, clip_len, heads)
    context = attend(prior, vision, clip_start, clip_len, heads, context)
    parts = spread(context, "head")
    frame = arrange(own, prior, clip_start, clip_len)
    sequence = project(frame, parts, outs, projector, text_rows, clip_start, clip_len)
    blocks = spread(sequence, "head")
    half = groups // 2
    near_keys, far_keys = tuple(range(half)), tuple(range(half, groups))
    query_sum, pair_sum, squares = near(blocks[:half], near_keys, layer)
    key_rows, value_rows, delta, scale = pair(blocks[half:], far_keys, layer, pair_sum, squares)
    carried = earlier_sum(delta, "ctx")
    query, intra = within(blocks[half:], far_keys, layer, query_sum, scale, key_rows, value_rows)
    return finish(query, intra, carried, state_in, head_gain)


def solution(mesh):
    placed = (
        P(("ctx", "head"), None),
        P(),
        P(),
        P("ctx", "head"),
        P(None, None, "head"),
        P("head", None),
        P(None, "head"),
        P(None, None, "head"),
        P("head"),
        P("head", None, None),
    )
    return jax.shard_map(
        local, mesh=mesh, in_specs=placed, out_specs=P("ctx", "head"), check_vma=False
    )
```

```python
import functools
import math

import jax
import jax.numpy as jnp
from jax import lax
from jax.experimental import pallas as pl
from jax.experimental.pallas import tpu as pltpu
from jax.sharding import PartitionSpec as P

VIT_HEADS = 16
HD = 128

EPS = 1e-06
LOW = -1e30
BLOCK = 128
SPLIT = 2
VMEM = pl.BlockSpec(memory_space=pltpu.VMEM)
HBM = pl.BlockSpec(memory_space=pltpu.HBM)
F32 = jnp.float32
BF16 = jnp.bfloat16


def dot(left, right):
    return jnp.dot(left, right, preferred_element_type=F32)


def dot_t(left, right):
    return lax.dot_general(left, right, (((1,), (1,)), ((), ())), preferred_element_type=F32)


def shifted(value, axis, steps):
    count = lax.axis_size(axis)
    return lax.ppermute(value, axis, [(source, source + steps) for source in range(count - steps)])


def swapped(value, axis, bit):
    count = lax.axis_size(axis)
    return lax.ppermute(value, axis, [(source, source ^ bit) for source in range(count)])


def widen(blocks, stride):
    count = lax.axis_size("head")
    while stride >= 1:
        for key in list(blocks):
            blocks[key ^ stride] = swapped(blocks[key], "head", stride)
        stride //= 2
    return [blocks[key] for key in range(count)]


def spread(value):
    return widen({0: value}, lax.axis_size("head") // 2)


def spread_prior(blocks):
    stride = lax.axis_size("head") // 2
    handed = {0: shifted(blocks[0], "ctx", 1), stride: shifted(blocks[stride], "ctx", 1)}
    return widen(handed, stride // 2)


def earlier_sum(value, axis):
    count = lax.axis_size(axis)
    place = lax.axis_index(axis)
    partner = swapped(value, axis, 1)
    total = value.astype(F32) + partner.astype(F32)
    before = jnp.where(place % 2 == 1, partner.astype(F32), 0.0)
    parts = [before]
    step = 1
    while 2 * step < count:
        arrived = shifted(total.astype(BF16), axis, 2 * step).astype(F32)
        parts.append(arrived)
        total = total + arrived
        step *= 2
    return sum(parts)


def fetch(tables, copies, semaphores):
    moves = [
        pltpu.make_async_copy(table, copy, semaphores.at[index])
        for index, (table, copy) in enumerate(zip(tables, copies))
    ]
    for move in moves:
        move.start()
    return moves


def table_scratch(*tables):
    return [pltpu.SMEM(table.shape, table.dtype) for table in tables] + [
        pltpu.SemaphoreType.DMA((len(tables),))
    ]


def clip_span(starts, lens, span, prior):
    place = lax.axis_index("ctx")
    if prior:
        source = jnp.maximum(place - 1, 0)
        shift = span - starts[source]
        length = jnp.where(place > 0, lens[source], 0)
    else:
        shift = -starts[place]
        length = lens[place]
    return shift, length, jnp.maximum(0, -shift), jnp.minimum(span, length - shift)


def clip_rows(rows, count, span):
    me = lax.axis_index("head")
    slot = lax.broadcasted_iota(jnp.int32, (1, span), 1)
    row = slot
    for key in range(count):
        inside = (slot >= key * rows) & (slot < (key + 1) * rows)
        row = jnp.where(inside, slot + ((me ^ key) - key) * rows, row)
    return row


def packed_shape(span, inner):
    whole = inner // 256 * 256
    return span + span * (inner - whole) // whole, whole


def pack(value):
    span, inner = value.shape
    whole = inner // 256 * 256
    groups = whole // (inner - whole)
    rows = span // groups
    tail = jnp.concatenate(
        [value[group * rows : (group + 1) * rows, whole:] for group in range(groups)], axis=1
    )
    return jnp.concatenate([value[:, :whole], tail], axis=0)


def unpack_tail(value, span):
    whole = value.shape[1]
    rows = value.shape[0] - span
    width = rows * whole // span
    return jnp.concatenate(
        [value[span:, group * width : (group + 1) * width] for group in range(span // rows)], axis=0
    )


def output_product(parts, weights, span):
    whole = parts[0].shape[1]
    left = jnp.concatenate(
        [part[:span, :] for part in parts] + [unpack_tail(part[...], span) for part in parts], axis=1
    )
    right = jnp.concatenate(
        [weight[:whole, :] for weight in weights] + [weight[whole:, :] for weight in weights], axis=0
    )
    return dot(left, right)


def attend_kernel(prior, heads, block, far_starts, far_lens, *refs):
    *refs, starts, lens, semaphores = refs
    moves = fetch((far_starts, far_lens), (starts, lens), semaphores)
    if prior:
        *refs, held_context = refs
    count = len(refs) - (6 if prior else 5)
    pieces = refs[:count]
    weights, *olds, result, queries, keys, values = refs[count:]
    context = olds[0] if prior else result
    rows, width = pieces[0].shape
    span = rows * count
    inner = weights.shape[0] // 3
    size = inner // heads
    if not prior:
        context[...] = jnp.zeros_like(context)
    row = clip_rows(rows, count, span)
    lane = lax.broadcasted_iota(jnp.int32, (1, inner), 1)
    owner = [(lane >= head * size) & (lane < (head + 1) * size) for head in range(heads)]
    groups = {}
    for head in range(heads):
        groups.setdefault(head * size // 128 * 128, []).append(head)

    if prior:
        for move in moves:
            move.wait()
        shift, length, first, last = clip_span(starts, lens, span, prior)

    @pl.when(last > first if prior else True)
    def _():
        frame = jnp.concatenate([piece[...] for piece in pieces], axis=0)
        wide = frame.astype(F32)
        scale = lax.rsqrt(jnp.sum(wide * wide, axis=-1, keepdims=True) * (1.0 / width) + EPS)
        full = dot_t(frame, weights[...])
        queries[...] = (full[:, :inner] * (scale * (size**-0.5 * math.log2(math.e)))).astype(BF16)
        keys[...] = (full[:, inner : 2 * inner] * scale).astype(BF16)
        values[...] = (full[:, 2 * inner :] * scale).astype(BF16)

    if not prior:
        for move in moves:
            move.wait()
        shift, length, first, last = clip_span(starts, lens, span, prior)

    def step(index, _):
        low = pl.multiple_of(index * block, block)
        place = low + lax.broadcasted_iota(jnp.int32, (block, 1), 0)
        live = (place >= first) & (place < last)
        pick = (place + shift == row) & live
        query = dot(jnp.where(pick, 1.0, 0.0).astype(BF16), queries[...])
        total = jnp.zeros((block, inner), F32)
        for base, members in groups.items():
            end = min(inner, base + 256)
            stack = jnp.concatenate(
                [jnp.where(owner[head], query, 0.0)[:, base:end].astype(BF16) for head in members], axis=0
            )
            scores = dot_t(stack, keys[:, base:end])
            scores = jnp.where(row < length, scores, LOW)
            powers = jnp.exp2(scores - jnp.max(scores, axis=-1, keepdims=True))
            mass = jnp.sum(powers, axis=-1, keepdims=True)
            mixed = dot(powers.astype(BF16), values[:, base:end]) / mass
            for place_in, head in enumerate(members):
                part = mixed[place_in * block : (place_in + 1) * block, :]
                sides = [part]
                if base:
                    sides = [jnp.zeros((block, base), F32)] + sides
                if end < inner:
                    sides = sides + [jnp.zeros((block, inner - end), F32)]
                total = jnp.where(owner[head], jnp.concatenate(sides, axis=1), total)
        here = pl.ds(low, block)
        if prior:
            context[here, :] = jnp.where(live, total, context[here, :].astype(F32)).astype(BF16)
        else:
            context[here, :] = total.astype(BF16)
        return 0

    if prior:
        held_context[...] = context[...]
        context = held_context
    lax.fori_loop(first // block, jnp.where(last > first, (last + block - 1) // block, 0), step, 0)
    if prior:
        result[...] = pack(context[...])


def attend(pieces, weights, starts, lens, heads, old=None):
    rows, _ = pieces[0].shape
    span = rows * len(pieces)
    inner = weights.shape[0] // 3
    olds = [] if old is None else [old]
    return pl.pallas_call(
        functools.partial(attend_kernel, old is not None, heads, min(BLOCK, span)),
        out_shape=jax.ShapeDtypeStruct(packed_shape(span, inner) if olds else (span, inner), BF16),
        in_specs=[HBM, HBM] + [VMEM] * (len(pieces) + 1 + len(olds)),
        out_specs=VMEM,
        scratch_shapes=[pltpu.VMEM((span, inner), BF16)] * (3 + len(olds)) + table_scratch(starts, lens),
        compiler_params=pltpu.CompilerParams(vmem_limit_bytes=16 * 2**20),
        cost_estimate=pl.CostEstimate(flops=5 * 10**9, bytes_accessed=4 * 10**6, transcendentals=10**6),
        name="attend_prior" if olds else "attend_own",
    )(starts, lens, *pieces, weights, *olds)


def warm_kernel(source, target):
    target[...] = source[...]


def warm(weights):
    return pl.pallas_call(
        warm_kernel,
        out_shape=jax.ShapeDtypeStruct(weights.shape, weights.dtype),
        in_specs=[VMEM],
        out_specs=VMEM,
        compiler_params=pltpu.CompilerParams(vmem_limit_bytes=6 * 2**20),
        cost_estimate=pl.CostEstimate(flops=10**9, bytes_accessed=4 * 10**6, transcendentals=0),
        name="warm",
    )(weights)


def arrange_kernel(far_starts, far_lens, *refs):
    *refs, starts, lens, semaphores = refs
    for move in fetch((far_starts, far_lens), (starts, lens), semaphores):
        move.wait()
    near_count = len(refs) - 1 - 2 * lax.axis_size("head")
    near_refs, refs = refs[: near_count], refs[near_count:]
    frame_out = refs[-1]
    count = (len(refs) - 1) // 2
    rows, _ = refs[0].shape
    span = rows * count
    row = clip_rows(rows, count, span)
    place = lax.broadcasted_iota(jnp.int32, (span, 1), 0)
    total = output_product(near_refs[: near_count // 2], near_refs[near_count // 2 :], span)
    for prior in (False, True):
        shift, length, _, _ = clip_span(starts, lens, span, prior)
        pick = (place + shift == row) & (row < length)
        frame = jnp.concatenate([piece[...] for piece in refs[prior * count : (prior + 1) * count]], axis=0)
        total = total + dot(jnp.where(pick, 1.0, 0.0).astype(BF16), frame)
    frame_out[...] = total


def arrange(own, prior, parts, outs, starts, lens):
    rows, width = own[0].shape
    span = rows * len(own)
    return pl.pallas_call(
        arrange_kernel,
        out_shape=jax.ShapeDtypeStruct((span, width), F32),
        in_specs=[HBM, HBM] + [VMEM] * (2 * len(own) + 2 * len(parts)),
        out_specs=VMEM,
        scratch_shapes=table_scratch(starts, lens),
        compiler_params=pltpu.CompilerParams(vmem_limit_bytes=16 * 2**20),
        cost_estimate=pl.CostEstimate(flops=2 * 10**9, bytes_accessed=3 * 10**6, transcendentals=0),
        name="arrange",
    )(starts, lens, *parts, *outs, *own, *prior)


def project_kernel(low, span, far_starts, far_lens, *refs):
    *refs, starts, lens, semaphores = refs
    moves = fetch((far_starts, far_lens), (starts, lens), semaphores)
    base, projector, text, *pieces, result = refs
    parts, weights = pieces[: len(pieces) // 2], pieces[len(pieces) // 2 :]
    rows = result.shape[0]
    here = slice(low, low + rows)
    whole = parts[0].shape[1]
    left = jnp.concatenate(
        [part[here, :] for part in parts] + [unpack_tail(part[...], span)[here] for part in parts], axis=1
    )
    right = jnp.concatenate(
        [weight[:whole, :] for weight in weights] + [weight[whole:, :] for weight in weights], axis=0
    )
    resid = base[here, :] + dot(left, right)
    scale = lax.rsqrt(jnp.mean(resid * resid, axis=-1, keepdims=True) + EPS)
    visual = dot((resid * scale).astype(BF16), projector[...]).astype(BF16)
    for move in moves:
        move.wait()
    _, _, own_first, own_last = clip_span(starts, lens, span, False)
    _, _, prior_first, prior_last = clip_span(starts, lens, span, True)
    place = low + lax.broadcasted_iota(jnp.int32, (rows, 1), 0)
    live = ((place >= own_first) & (place < own_last)) | (
        (place >= prior_first) & (place < prior_last)
    )
    result[...] = jnp.where(live, visual, text[here, :])


def project(index, count, base, parts, outs, projector, text, starts, lens):
    span, columns = text.shape
    rows = span // count
    return pl.pallas_call(
        functools.partial(project_kernel, index * rows, span),
        out_shape=jax.ShapeDtypeStruct((rows, columns), BF16),
        in_specs=[HBM, HBM] + [VMEM] * (3 + 2 * len(parts)),
        out_specs=VMEM,
        scratch_shapes=table_scratch(starts, lens),
        compiler_params=pltpu.CompilerParams(vmem_limit_bytes=12 * 2**20),
        cost_estimate=pl.CostEstimate(flops=10**9, bytes_accessed=2 * 10**6, transcendentals=0),
    )(starts, lens, base, projector, text, *parts, *outs)


def held(weights, part, key, depth):
    start = pl.multiple_of((lax.axis_index("head") ^ key) * depth, depth)
    return weights[part, pl.ds(start, depth), :]


def near_kernel(keys, weights, *refs):
    count = len(keys)
    pieces = refs[:count]
    query_sum, pair_sum, squares = refs[count:]
    norm = 0.0
    for piece in pieces:
        wide = piece[...].astype(F32)
        norm = norm + jnp.sum(wide * wide, axis=-1, keepdims=True)
    squares[...] = jnp.broadcast_to(norm, squares.shape)
    for part in range(3):
        total = 0.0
        for index in range(count):
            total = total + dot(pieces[index][...], held(weights, part, keys[index], pieces[index].shape[1]))
        if part == 0:
            query_sum[...] = total
        else:
            pair_sum[part - 1] = total


def near(pieces, keys, weights):
    span, _ = pieces[0].shape
    columns = weights.shape[2]
    return pl.pallas_call(
        functools.partial(near_kernel, keys),
        out_shape=(
            jax.ShapeDtypeStruct((span, columns), F32),
            jax.ShapeDtypeStruct((2, span, columns), F32),
            jax.ShapeDtypeStruct((span, HD), F32),
        ),
        in_specs=[VMEM] * (1 + len(pieces)),
        out_specs=(VMEM, VMEM, VMEM),
        compiler_params=pltpu.CompilerParams(vmem_limit_bytes=12 * 2**20),
        cost_estimate=pl.CostEstimate(flops=3 * 10**9, bytes_accessed=7 * 10**6, transcendentals=0),
    )(weights, *pieces)


def pair_kernel(keys, total_depth, weights, pair_sum, squares, *refs):
    count = len(keys)
    pieces = refs[:count]
    *olds, key_out, value_out, delta, scale_out = refs[count:]
    norm = squares[:, :1]
    for piece in pieces:
        wide = piece[...].astype(F32)
        norm = norm + jnp.sum(wide * wide, axis=-1, keepdims=True)
    scale = lax.rsqrt(norm * (1.0 / total_depth) + EPS)
    scale_out[...] = jnp.broadcast_to(scale, scale_out.shape)
    for part, out in ((0, key_out), (1, value_out)):
        total = pair_sum[part]
        for index in range(count):
            total = total + dot(pieces[index][...], held(weights, part + 1, keys[index], pieces[index].shape[1]))
        out[...] = (total * scale).astype(BF16)
    for head in range(delta.shape[0]):
        lanes = slice(head * HD, (head + 1) * HD)
        product = lax.dot_general(
            key_out[:, lanes], value_out[:, lanes], (((0,), (0,)), ((), ())), preferred_element_type=F32
        )
        if olds:
            product = product + olds[0][head]
        delta[head] = product.astype(delta.dtype)


def pair(kind, pieces, keys, weights, pair_sum, squares, olds):
    span, _ = pieces[0].shape
    columns = weights.shape[2]
    return pl.pallas_call(
        functools.partial(pair_kernel, keys, weights.shape[1]),
        out_shape=(
            jax.ShapeDtypeStruct((span, columns), BF16),
            jax.ShapeDtypeStruct((span, columns), BF16),
            jax.ShapeDtypeStruct((columns // HD, HD, HD), kind),
            jax.ShapeDtypeStruct((span, HD), F32),
        ),
        in_specs=[VMEM] * (3 + len(pieces) + len(olds)),
        out_specs=(VMEM,) * 4,
        compiler_params=pltpu.CompilerParams(vmem_limit_bytes=12 * 2**20),
        cost_estimate=pl.CostEstimate(flops=3 * 10**9, bytes_accessed=7 * 10**6, transcendentals=0),
    )(weights, pair_sum, squares, *pieces, *olds)


def within_kernel(keys, groups, weights, *refs):
    count = len(keys)
    sizes = (groups, groups, groups, groups, groups * count)
    lists, at = [], 0
    for size in sizes:
        lists.append(refs[at : at + size])
        at += size
    query_sums, scales, key_ins, value_ins, pieces = lists
    query_out, intra, buffers, semaphores = refs[at:]
    rows, depth = pieces[0].shape
    starts = [pl.multiple_of((lax.axis_index("head") ^ key) * depth, depth) for key in keys]
    moves = fetch(
        [weights.at[0, pl.ds(start, depth), :] for start in starts],
        [buffers.at[index] for index in range(count)],
        semaphores,
    )
    for move in moves:
        move.wait()
    causal = lax.broadcasted_iota(jnp.int32, (rows, rows), 0) >= lax.broadcasted_iota(
        jnp.int32, (rows, rows), 1
    )
    for group in range(groups):
        here = slice(group * rows, (group + 1) * rows)
        total = query_sums[group][...]
        for index in range(count):
            total = total + dot(pieces[group * count + index][...], buffers[index])
        query_out[here, :] = (total * scales[group][:, :1]).astype(BF16)
        for head in range(query_out.shape[1] // HD):
            lanes = slice(head * HD, (head + 1) * HD)
            query = query_out[here, lanes]
            corner = dot_t(query, key_ins[group][:, lanes])
            corner = jnp.where(causal, corner, 0.0).astype(BF16)
            total = dot(corner, value_ins[group][:, lanes])
            for earlier in range(group):
                left = dot_t(query, key_ins[earlier][:, lanes]).astype(BF16)
                total = total + dot(left, value_ins[earlier][:, lanes])
            intra[here, lanes] = total


def within(pieces, keys, weights, query_sums, scales, key_ins, value_ins):
    rows, depth = pieces[0].shape
    groups = len(query_sums)
    columns = weights.shape[2]
    return pl.pallas_call(
        functools.partial(within_kernel, keys, groups),
        out_shape=(
            jax.ShapeDtypeStruct((groups * rows, columns), BF16),
            jax.ShapeDtypeStruct((groups * rows, columns), F32),
        ),
        in_specs=[HBM] + [VMEM] * (4 * groups + len(pieces)),
        out_specs=(VMEM,) * 2,
        scratch_shapes=[
            pltpu.VMEM((len(keys), depth, columns), BF16),
            pltpu.SemaphoreType.DMA((len(keys),)),
        ],
        compiler_params=pltpu.CompilerParams(vmem_limit_bytes=12 * 2**20),
        cost_estimate=pl.CostEstimate(flops=3 * 10**9, bytes_accessed=5 * 10**6, transcendentals=0),
        name="within",
    )(weights, *query_sums, *scales, *key_ins, *value_ins, *pieces)


def finish_kernel(query, intra, carried, state, gain, out):
    for head in range(state.shape[0]):
        lanes = slice(head * HD, (head + 1) * HD)
        whole = (carried[head] + state[head]).astype(BF16)
        lin = intra[:, lanes] + dot(query[:, lanes], whole)
        scale = lax.rsqrt(jnp.mean(lin * lin, axis=-1, keepdims=True) + EPS)
        out[:, lanes] = (lin * scale * gain[:, lanes]).astype(BF16)


def finish(query, intra, carried, state, gain):
    return pl.pallas_call(
        finish_kernel,
        out_shape=jax.ShapeDtypeStruct(query.shape, BF16),
        in_specs=[VMEM] * 5,
        out_specs=VMEM,
        compiler_params=pltpu.CompilerParams(vmem_limit_bytes=8 * 2**20),
        cost_estimate=pl.CostEstimate(flops=10**8, bytes_accessed=3 * 10**6, transcendentals=0),
        name="finish",
    )(query, intra, carried, state, gain.reshape(1, -1))


def program(
    patches,
    clip_start,
    clip_len,
    text_rows,
    vision_qkv,
    vision_out,
    projector,
    layer_qkv,
    head_gain,
    state_in,
):
    groups = lax.axis_size("head")
    heads = VIT_HEADS // groups
    own = spread(patches)
    prior = spread_prior(own)
    outs = spread(vision_out)
    vision = jnp.transpose(vision_qkv, (1, 2, 0)).reshape(-1, vision_qkv.shape[0])
    layer = jnp.transpose(layer_qkv, (1, 0, 2))
    vision = warm(vision)
    context = attend(own, vision, clip_start, clip_len, heads)
    context = attend(prior, vision, clip_start, clip_len, heads, context)
    parts = spread(context)
    half = groups // 2
    near_keys, far_keys = tuple(range(half)), tuple(range(half, groups))
    base = arrange(own, prior, parts[:half], outs[:half], clip_start, clip_len)
    query_sums, scales, key_rows, value_rows, pieces, old = [], [], [], [], [], []
    for index in range(SPLIT):
        sequence = project(
            index, SPLIT, base, parts[half:], outs[half:], projector, text_rows, clip_start, clip_len
        )
        blocks = spread(sequence)
        query_sum, pair_sum, squares = near(blocks[:half], near_keys, layer)
        kind = BF16 if index == SPLIT - 1 else F32
        key_row, value_row, delta, scale = pair(kind, blocks[half:], far_keys, layer, pair_sum, squares, old)
        old = [delta]
        query_sums.append(query_sum)
        scales.append(scale)
        key_rows.append(key_row)
        value_rows.append(value_row)
        pieces += blocks[half:]
    carried = earlier_sum(delta, "ctx")
    query, intra = within(pieces, far_keys, layer, query_sums, scales, key_rows, value_rows)
    return finish(query, intra, carried, state_in, head_gain)


def solution(mesh):
    placed = (
        P(("ctx", "head"), None),
        P(),
        P(),
        P("ctx", "head"),
        P(None, None, "head"),
        P("head", None),
        P(None, "head"),
        P(None, None, "head"),
        P("head"),
        P("head", None, None),
    )
    return jax.shard_map(program, mesh=mesh, in_specs=placed, out_specs=P("ctx", "head"), check_vma=False)
```

```python
import functools
import math

import jax
import jax.numpy as jnp
from jax import lax
from jax.experimental import pallas as pl
from jax.experimental.pallas import tpu as pltpu
from jax.sharding import PartitionSpec as P

VIT_HEADS = 16
HD = 128

EPS = 1e-06
LOW = -1e30
BLOCK = 128
SHARES = (2, 2)
VMEM = pl.BlockSpec(memory_space=pltpu.VMEM)
HBM = pl.BlockSpec(memory_space=pltpu.HBM)
F32 = jnp.float32
BF16 = jnp.bfloat16


def dot(left, right):
    return jnp.dot(left, right, preferred_element_type=F32)


def dot_t(left, right):
    return lax.dot_general(left, right, (((1,), (1,)), ((), ())), preferred_element_type=F32)


def shifted(value, axis, steps):
    count = lax.axis_size(axis)
    return lax.ppermute(value, axis, [(source, source + steps) for source in range(count - steps)])


def swapped(value, axis, bit):
    count = lax.axis_size(axis)
    return lax.ppermute(value, axis, [(source, source ^ bit) for source in range(count)])


def widen(blocks, stride):
    count = lax.axis_size("head")
    while stride >= 1:
        for key in list(blocks):
            blocks[key ^ stride] = swapped(blocks[key], "head", stride)
        stride //= 2
    return [blocks[key] for key in range(count)]


def spread(value):
    return widen({0: value}, lax.axis_size("head") // 2)


def spread_prior(blocks):
    stride = lax.axis_size("head") // 2
    handed = {0: shifted(blocks[0], "ctx", 1), stride: shifted(blocks[stride], "ctx", 1)}
    return widen(handed, stride // 2)


def earlier_sum(value, axis):
    count = lax.axis_size(axis)
    place = lax.axis_index(axis)
    total = value.astype(F32)
    before = jnp.zeros_like(total)
    bit = 1
    while bit < count:
        slim = total.astype(BF16)
        if 2 * bit < count:
            other = swapped(slim, axis, bit).astype(F32)
        else:
            ahead = [(source, source + bit) for source in range(count - bit)]
            other = lax.ppermute(slim, axis, ahead).astype(F32)
        before = before + jnp.where(place & bit != 0, other, 0.0)
        total = total + other
        bit *= 2
    return before


def fetch(tables, copies, semaphores):
    moves = [
        pltpu.make_async_copy(table, copy, semaphores.at[index])
        for index, (table, copy) in enumerate(zip(tables, copies))
    ]
    for move in moves:
        move.start()
    return moves


def table_scratch(*tables):
    return [pltpu.SMEM(table.shape, table.dtype) for table in tables] + [
        pltpu.SemaphoreType.DMA((len(tables),))
    ]


def clip_span(starts, lens, span, prior):
    place = lax.axis_index("ctx")
    if prior:
        source = jnp.maximum(place - 1, 0)
        shift = span - starts[source]
        length = jnp.where(place > 0, lens[source], 0)
    else:
        shift = -starts[place]
        length = lens[place]
    return shift, length, jnp.maximum(0, -shift), jnp.minimum(span, length - shift)


def clip_rows(rows, count, span):
    me = lax.axis_index("head")
    slot = lax.broadcasted_iota(jnp.int32, (1, span), 1)
    row = slot
    for key in range(count):
        inside = (slot >= key * rows) & (slot < (key + 1) * rows)
        row = jnp.where(inside, slot + ((me ^ key) - key) * rows, row)
    return row


def packed_shape(span, inner):
    whole = inner // 256 * 256
    return span + span * (inner - whole) // whole, whole


def pack(value):
    span, inner = value.shape
    whole = inner // 256 * 256
    groups = whole // (inner - whole)
    rows = span // groups
    tail = jnp.concatenate(
        [value[group * rows : (group + 1) * rows, whole:] for group in range(groups)], axis=1
    )
    return jnp.concatenate([value[:, :whole], tail], axis=0)


def unpack_tail(value, span):
    whole = value.shape[1]
    rows = value.shape[0] - span
    width = rows * whole // span
    return jnp.concatenate(
        [value[span:, group * width : (group + 1) * width] for group in range(span // rows)], axis=0
    )


def output_product(parts, weights, span):
    whole = parts[0].shape[1]
    left = jnp.concatenate(
        [part[:span, :] for part in parts] + [unpack_tail(part[...], span) for part in parts], axis=1
    )
    right = jnp.concatenate(
        [weight[:whole, :] for weight in weights] + [weight[whole:, :] for weight in weights], axis=0
    )
    return dot(left, right)


def mix(pieces, weights, size):
    frame = jnp.concatenate([piece[...] for piece in pieces], axis=0)
    inner = weights.shape[0] // 3
    wide = frame.astype(F32)
    scale = lax.rsqrt(jnp.mean(wide * wide, axis=-1, keepdims=True) + EPS)
    full = dot_t(frame, weights[...])
    return (
        (full[:, :inner] * (scale * (size**-0.5 * math.log2(math.e)))).astype(BF16),
        (full[:, inner : 2 * inner] * scale).astype(BF16),
        (full[:, 2 * inner :] * scale).astype(BF16),
    )


def mix_kernel(size, *refs):
    *pieces, weights, queries, keys, values = refs
    queries[...], keys[...], values[...] = mix(pieces, weights, size)


def mix_rows(pieces, weights, heads):
    rows = pieces[0].shape[0] * len(pieces)
    inner = weights.shape[0] // 3
    return pl.pallas_call(
        functools.partial(mix_kernel, inner // heads),
        out_shape=(jax.ShapeDtypeStruct((rows, inner), BF16),) * 3,
        in_specs=[VMEM] * (len(pieces) + 1),
        out_specs=(VMEM,) * 3,
        compiler_params=pltpu.CompilerParams(vmem_limit_bytes=10 * 2**20),
        cost_estimate=pl.CostEstimate(flops=10**9, bytes_accessed=4 * 10**6, transcendentals=0),
        name="prior_mix",
    )(*pieces, weights)


def attend_kernel(prior, count, heads, block, far_starts, far_lens, *refs):
    *refs, starts, lens, semaphores = refs
    moves = fetch((far_starts, far_lens), (starts, lens), semaphores)
    if prior:
        *refs, old, result, queries, keys, values, context = refs
        *pieces, weights, near_queries, near_keys, near_values = refs
    else:
        *pieces, weights, context, queries, keys, values = refs
    rows, _ = pieces[0].shape
    span = rows * count
    inner = weights.shape[0] // 3
    size = inner // heads
    row = clip_rows(rows, count, span)
    lane = lax.broadcasted_iota(jnp.int32, (1, inner), 1)
    owner = [(lane >= head * size) & (lane < (head + 1) * size) for head in range(heads)]
    groups = {}
    for head in range(heads):
        groups.setdefault(head * size // 128 * 128, []).append(head)

    def fill(first_row):
        queries[first_row:, :], keys[first_row:, :], values[first_row:, :] = mix(pieces, weights, size)

    if prior:
        context[...] = old[...]
        for move in moves:
            move.wait()
        shift, length, first, last = clip_span(starts, lens, span, prior)

        @pl.when(last > first)
        def _():
            held_rows = near_queries.shape[0]
            queries[:held_rows, :] = near_queries[...]
            keys[:held_rows, :] = near_keys[...]
            values[:held_rows, :] = near_values[...]
            fill(held_rows)

    else:
        context[...] = jnp.zeros_like(context)
        fill(0)
        for move in moves:
            move.wait()
        shift, length, first, last = clip_span(starts, lens, span, prior)

    def step(index, _):
        low = pl.multiple_of(index * block, block)
        place = low + lax.broadcasted_iota(jnp.int32, (block, 1), 0)
        live = (place >= first) & (place < last)
        pick = (place + shift == row) & live
        query = dot(jnp.where(pick, 1.0, 0.0).astype(BF16), queries[...])
        total = jnp.zeros((block, inner), F32)
        for base, members in groups.items():
            end = min(inner, base + 256)
            stack = jnp.concatenate(
                [jnp.where(owner[head], query, 0.0)[:, base:end].astype(BF16) for head in members], axis=0
            )
            scores = dot_t(stack, keys[:, base:end])
            scores = jnp.where(row < length, scores, LOW)
            powers = jnp.exp2(scores - jnp.max(scores, axis=-1, keepdims=True))
            mass = jnp.sum(powers, axis=-1, keepdims=True)
            mixed = dot(powers.astype(BF16), values[:, base:end]) / mass
            for place_in, head in enumerate(members):
                part = mixed[place_in * block : (place_in + 1) * block, :]
                sides = [part]
                if base:
                    sides = [jnp.zeros((block, base), F32)] + sides
                if end < inner:
                    sides = sides + [jnp.zeros((block, inner - end), F32)]
                total = jnp.where(owner[head], jnp.concatenate(sides, axis=1), total)
        here = pl.ds(low, block)
        if prior:
            context[here, :] = jnp.where(live, total, context[here, :].astype(F32)).astype(BF16)
        else:
            context[here, :] = total.astype(BF16)
        return 0

    lax.fori_loop(first // block, jnp.where(last > first, (last + block - 1) // block, 0), step, 0)
    if prior:
        result[...] = pack(context[...])


def attend(pieces, weights, starts, lens, heads, near_rows=(), old=()):
    rows, _ = pieces[0].shape
    held_rows = near_rows[0].shape[0] if near_rows else 0
    span = rows * len(pieces) + held_rows
    inner = weights.shape[0] // 3
    extra = [*near_rows, *old]
    return pl.pallas_call(
        functools.partial(attend_kernel, len(old) > 0, span // rows, heads, min(BLOCK, span)),
        out_shape=jax.ShapeDtypeStruct(packed_shape(span, inner) if old else (span, inner), BF16),
        in_specs=[HBM, HBM] + [VMEM] * (len(pieces) + 1 + len(extra)),
        out_specs=VMEM,
        scratch_shapes=[pltpu.VMEM((span, inner), BF16)] * (3 + len(old)) + table_scratch(starts, lens),
        compiler_params=pltpu.CompilerParams(vmem_limit_bytes=16 * 2**20),
        cost_estimate=pl.CostEstimate(flops=5 * 10**9, bytes_accessed=4 * 10**6, transcendentals=10**6),
        name="attend_prior" if old else "attend_own",
    )(starts, lens, *pieces, weights, *extra)


def warm_kernel(source, target):
    target[...] = source[...]


def warm(weights):
    return pl.pallas_call(
        warm_kernel,
        out_shape=jax.ShapeDtypeStruct(weights.shape, weights.dtype),
        in_specs=[VMEM],
        out_specs=VMEM,
        compiler_params=pltpu.CompilerParams(vmem_limit_bytes=6 * 2**20),
        cost_estimate=pl.CostEstimate(flops=10**9, bytes_accessed=4 * 10**6, transcendentals=0),
        name="warm",
    )(weights)


def arrange_kernel(far_starts, far_lens, *refs):
    *refs, starts, lens, semaphores = refs
    for move in fetch((far_starts, far_lens), (starts, lens), semaphores):
        move.wait()
    near_count = len(refs) - 1 - 2 * lax.axis_size("head")
    near_refs, refs = refs[: near_count], refs[near_count:]
    frame_out = refs[-1]
    count = (len(refs) - 1) // 2
    rows, _ = refs[0].shape
    span = rows * count
    row = clip_rows(rows, count, span)
    place = lax.broadcasted_iota(jnp.int32, (span, 1), 0)
    total = output_product(near_refs[: near_count // 2], near_refs[near_count // 2 :], span)
    for prior in (False, True):
        shift, length, _, _ = clip_span(starts, lens, span, prior)
        pick = (place + shift == row) & (row < length)
        frame = jnp.concatenate([piece[...] for piece in refs[prior * count : (prior + 1) * count]], axis=0)
        total = total + dot(jnp.where(pick, 1.0, 0.0).astype(BF16), frame)
    frame_out[...] = total


def arrange(own, prior, parts, outs, starts, lens):
    rows, width = own[0].shape
    span = rows * len(own)
    return pl.pallas_call(
        arrange_kernel,
        out_shape=jax.ShapeDtypeStruct((span, width), F32),
        in_specs=[HBM, HBM] + [VMEM] * (2 * len(own) + 2 * len(parts)),
        out_specs=VMEM,
        scratch_shapes=table_scratch(starts, lens),
        compiler_params=pltpu.CompilerParams(vmem_limit_bytes=16 * 2**20),
        cost_estimate=pl.CostEstimate(flops=2 * 10**9, bytes_accessed=3 * 10**6, transcendentals=0),
        name="arrange",
    )(starts, lens, *parts, *outs, *own, *prior)


def project_kernel(low, span, far_starts, far_lens, *refs):
    *refs, starts, lens, semaphores = refs
    moves = fetch((far_starts, far_lens), (starts, lens), semaphores)
    base, projector, text, *pieces, result = refs
    parts, weights = pieces[: len(pieces) // 2], pieces[len(pieces) // 2 :]
    rows = result.shape[0]
    here = slice(low, low + rows)
    whole = parts[0].shape[1]
    left = jnp.concatenate(
        [part[here, :] for part in parts] + [unpack_tail(part[...], span)[here] for part in parts], axis=1
    )
    right = jnp.concatenate(
        [weight[:whole, :] for weight in weights] + [weight[whole:, :] for weight in weights], axis=0
    )
    resid = base[here, :] + dot(left, right)
    scale = lax.rsqrt(jnp.mean(resid * resid, axis=-1, keepdims=True) + EPS)
    visual = dot((resid * scale).astype(BF16), projector[...]).astype(BF16)
    for move in moves:
        move.wait()
    _, _, own_first, own_last = clip_span(starts, lens, span, False)
    _, _, prior_first, prior_last = clip_span(starts, lens, span, True)
    place = low + lax.broadcasted_iota(jnp.int32, (rows, 1), 0)
    live = ((place >= own_first) & (place < own_last)) | (
        (place >= prior_first) & (place < prior_last)
    )
    result[...] = jnp.where(live, visual, text[here, :])


def project(low, rows, base, parts, outs, projector, text, starts, lens):
    span, columns = text.shape
    return pl.pallas_call(
        functools.partial(project_kernel, low, span),
        out_shape=jax.ShapeDtypeStruct((rows, columns), BF16),
        in_specs=[HBM, HBM] + [VMEM] * (3 + 2 * len(parts)),
        out_specs=VMEM,
        scratch_shapes=table_scratch(starts, lens),
        compiler_params=pltpu.CompilerParams(vmem_limit_bytes=12 * 2**20),
        cost_estimate=pl.CostEstimate(flops=10**9, bytes_accessed=2 * 10**6, transcendentals=0),
    )(starts, lens, base, projector, text, *parts, *outs)


def held(weights, part, key, depth):
    start = pl.multiple_of((lax.axis_index("head") ^ key) * depth, depth)
    return weights[part, pl.ds(start, depth), :]


def near_kernel(keys, weights, *refs):
    count = len(keys)
    pieces = refs[:count]
    query_sum, pair_sum, squares = refs[count:]
    norm = 0.0
    for piece in pieces:
        wide = piece[...].astype(F32)
        norm = norm + jnp.sum(wide * wide, axis=-1, keepdims=True)
    squares[...] = jnp.broadcast_to(norm, squares.shape)
    for part in range(3):
        total = 0.0
        for index in range(count):
            total = total + dot(pieces[index][...], held(weights, part, keys[index], pieces[index].shape[1]))
        if part == 0:
            query_sum[...] = total
        else:
            pair_sum[part - 1] = total


def near(pieces, keys, weights):
    span, _ = pieces[0].shape
    columns = weights.shape[2]
    return pl.pallas_call(
        functools.partial(near_kernel, keys),
        out_shape=(
            jax.ShapeDtypeStruct((span, columns), F32),
            jax.ShapeDtypeStruct((2, span, columns), F32),
            jax.ShapeDtypeStruct((span, HD), F32),
        ),
        in_specs=[VMEM] * (1 + len(pieces)),
        out_specs=(VMEM, VMEM, VMEM),
        compiler_params=pltpu.CompilerParams(vmem_limit_bytes=12 * 2**20),
        cost_estimate=pl.CostEstimate(flops=3 * 10**9, bytes_accessed=7 * 10**6, transcendentals=0),
    )(weights, *pieces)


def pair_kernel(keys, total_depth, weights, pair_sum, squares, *refs):
    count = len(keys)
    pieces = refs[:count]
    *olds, key_out, value_out, delta, scale_out = refs[count:]
    norm = squares[:, :1]
    for piece in pieces:
        wide = piece[...].astype(F32)
        norm = norm + jnp.sum(wide * wide, axis=-1, keepdims=True)
    scale = lax.rsqrt(norm * (1.0 / total_depth) + EPS)
    scale_out[...] = jnp.broadcast_to(scale, scale_out.shape)
    for part, out in ((0, key_out), (1, value_out)):
        total = pair_sum[part]
        for index in range(count):
            total = total + dot(pieces[index][...], held(weights, part + 1, keys[index], pieces[index].shape[1]))
        out[...] = (total * scale).astype(BF16)
    for head in range(delta.shape[0]):
        lanes = slice(head * HD, (head + 1) * HD)
        product = lax.dot_general(
            key_out[:, lanes], value_out[:, lanes], (((0,), (0,)), ((), ())), preferred_element_type=F32
        )
        if olds:
            product = product + olds[0][head]
        delta[head] = product.astype(delta.dtype)


def pair(kind, pieces, keys, weights, pair_sum, squares, olds):
    span, _ = pieces[0].shape
    columns = weights.shape[2]
    return pl.pallas_call(
        functools.partial(pair_kernel, keys, weights.shape[1]),
        out_shape=(
            jax.ShapeDtypeStruct((span, columns), BF16),
            jax.ShapeDtypeStruct((span, columns), BF16),
            jax.ShapeDtypeStruct((columns // HD, HD, HD), kind),
            jax.ShapeDtypeStruct((span, HD), F32),
        ),
        in_specs=[VMEM] * (3 + len(pieces) + len(olds)),
        out_specs=(VMEM,) * 4,
        compiler_params=pltpu.CompilerParams(vmem_limit_bytes=12 * 2**20),
        cost_estimate=pl.CostEstimate(flops=3 * 10**9, bytes_accessed=7 * 10**6, transcendentals=0),
    )(weights, pair_sum, squares, *pieces, *olds)


def within_kernel(keys, groups, weights, *refs):
    count = len(keys)
    sizes = (groups, groups, groups, groups, groups * count)
    lists, at = [], 0
    for size in sizes:
        lists.append(refs[at : at + size])
        at += size
    query_sums, scales, key_ins, value_ins, pieces = lists
    query_out, intra, buffers, semaphores = refs[at:]
    depth = pieces[0].shape[1]
    starts = [pl.multiple_of((lax.axis_index("head") ^ key) * depth, depth) for key in keys]
    moves = fetch(
        [weights.at[0, pl.ds(start, depth), :] for start in starts],
        [buffers.at[index] for index in range(count)],
        semaphores,
    )
    for move in moves:
        move.wait()
    low = 0
    for group in range(groups):
        rows = query_sums[group].shape[0]
        here = slice(low, low + rows)
        low += rows
        causal = lax.broadcasted_iota(jnp.int32, (rows, rows), 0) >= lax.broadcasted_iota(
            jnp.int32, (rows, rows), 1
        )
        total = query_sums[group][...]
        for index in range(count):
            total = total + dot(pieces[group * count + index][...], buffers[index])
        query_out[here, :] = (total * scales[group][:, :1]).astype(BF16)
        for head in range(query_out.shape[1] // HD):
            lanes = slice(head * HD, (head + 1) * HD)
            query = query_out[here, lanes]
            corner = dot_t(query, key_ins[group][:, lanes])
            corner = jnp.where(causal, corner, 0.0).astype(BF16)
            total = dot(corner, value_ins[group][:, lanes])
            for earlier in range(group):
                left = dot_t(query, key_ins[earlier][:, lanes]).astype(BF16)
                total = total + dot(left, value_ins[earlier][:, lanes])
            intra[here, lanes] = total


def within(pieces, keys, weights, query_sums, scales, key_ins, value_ins):
    depth = pieces[0].shape[1]
    groups = len(query_sums)
    columns = weights.shape[2]
    span = sum(query_sum.shape[0] for query_sum in query_sums)
    return pl.pallas_call(
        functools.partial(within_kernel, keys, groups),
        out_shape=(
            jax.ShapeDtypeStruct((span, columns), BF16),
            jax.ShapeDtypeStruct((span, columns), F32),
        ),
        in_specs=[HBM] + [VMEM] * (4 * groups + len(pieces)),
        out_specs=(VMEM,) * 2,
        scratch_shapes=[
            pltpu.VMEM((len(keys), depth, columns), BF16),
            pltpu.SemaphoreType.DMA((len(keys),)),
        ],
        compiler_params=pltpu.CompilerParams(vmem_limit_bytes=12 * 2**20),
        cost_estimate=pl.CostEstimate(flops=3 * 10**9, bytes_accessed=5 * 10**6, transcendentals=0),
        name="within",
    )(weights, *query_sums, *scales, *key_ins, *value_ins, *pieces)


def finish_kernel(query, intra, carried, state, gain, out):
    for head in range(state.shape[0]):
        lanes = slice(head * HD, (head + 1) * HD)
        whole = (carried[head] + state[head]).astype(BF16)
        lin = intra[:, lanes] + dot(query[:, lanes], whole)
        scale = lax.rsqrt(jnp.mean(lin * lin, axis=-1, keepdims=True) + EPS)
        out[:, lanes] = (lin * scale * gain[:, lanes]).astype(BF16)


def finish(query, intra, carried, state, gain):
    return pl.pallas_call(
        finish_kernel,
        out_shape=jax.ShapeDtypeStruct(query.shape, BF16),
        in_specs=[VMEM] * 5,
        out_specs=VMEM,
        compiler_params=pltpu.CompilerParams(vmem_limit_bytes=8 * 2**20),
        cost_estimate=pl.CostEstimate(flops=10**8, bytes_accessed=3 * 10**6, transcendentals=0),
        name="finish",
    )(query, intra, carried, state, gain.reshape(1, -1))


def program(
    patches,
    clip_start,
    clip_len,
    text_rows,
    vision_qkv,
    vision_out,
    projector,
    layer_qkv,
    head_gain,
    state_in,
):
    groups = lax.axis_size("head")
    heads = VIT_HEADS // groups
    own = spread(patches)
    prior = spread_prior(own)
    outs = spread(vision_out)
    vision = jnp.transpose(vision_qkv, (1, 2, 0)).reshape(-1, vision_qkv.shape[0])
    layer = jnp.transpose(layer_qkv, (1, 0, 2))
    vision = warm(vision)
    context = attend(own, vision, clip_start, clip_len, heads)
    half = groups // 2
    near_rows = mix_rows(prior[:half], vision, heads)
    context = attend(prior[half:], vision, clip_start, clip_len, heads, near_rows, [context])
    parts = spread(context)
    near_keys, far_keys = tuple(range(half)), tuple(range(half, groups))
    base = arrange(own, prior, parts[:half], outs[:half], clip_start, clip_len)
    query_sums, scales, key_rows, value_rows, pieces, old = [], [], [], [], [], []
    low = 0
    for index, share in enumerate(SHARES):
        rows = text_rows.shape[0] // share
        sequence = project(low, rows, base, parts[half:], outs[half:], projector, text_rows, clip_start, clip_len)
        low += rows
        blocks = spread(sequence)
        query_sum, pair_sum, squares = near(blocks[:half], near_keys, layer)
        kind = BF16 if index == len(SHARES) - 1 else F32
        key_row, value_row, delta, scale = pair(kind, blocks[half:], far_keys, layer, pair_sum, squares, old)
        old = [delta]
        query_sums.append(query_sum)
        scales.append(scale)
        key_rows.append(key_row)
        value_rows.append(value_row)
        pieces += blocks[half:]
    carried = earlier_sum(delta, "ctx")
    query, intra = within(pieces, far_keys, layer, query_sums, scales, key_rows, value_rows)
    return finish(query, intra, carried, state_in, head_gain)


def solution(mesh):
    placed = (
        P(("ctx", "head"), None),
        P(),
        P(),
        P("ctx", "head"),
        P(None, None, "head"),
        P("head", None),
        P(None, "head"),
        P(None, None, "head"),
        P("head"),
        P("head", None, None),
    )
    return jax.shard_map(program, mesh=mesh, in_specs=placed, out_specs=P("ctx", "head"), check_vma=False)
```

```python
import functools
import math

import jax
import jax.numpy as jnp
from jax import lax
from jax.experimental import pallas as pl
from jax.experimental.pallas import tpu as pltpu
from jax.sharding import PartitionSpec as P

VIT_HEADS = 16
HD = 128

EPS = 1e-06
LOW = -1e30
BLOCK = 128
SHARES = (2, 2)
VMEM = pl.BlockSpec(memory_space=pltpu.VMEM)
HBM = pl.BlockSpec(memory_space=pltpu.HBM)
F32 = jnp.float32
BF16 = jnp.bfloat16


def dot(left, right):
    return jnp.dot(left, right, preferred_element_type=F32)


def dot_t(left, right):
    return lax.dot_general(left, right, (((1,), (1,)), ((), ())), preferred_element_type=F32)


def shifted(value, axis, steps):
    count = lax.axis_size(axis)
    return lax.ppermute(value, axis, [(source, source + steps) for source in range(count - steps)])


def swapped(value, axis, bit):
    count = lax.axis_size(axis)
    return lax.ppermute(value, axis, [(source, source ^ bit) for source in range(count)])


def widen(blocks, stride):
    count = lax.axis_size("head")
    while stride >= 1:
        for key in list(blocks):
            blocks[key ^ stride] = swapped(blocks[key], "head", stride)
        stride //= 2
    return [blocks[key] for key in range(count)]


def spread(value):
    return widen({0: value}, lax.axis_size("head") // 2)


def spread_prior(blocks):
    stride = lax.axis_size("head") // 2
    handed = {0: shifted(blocks[0], "ctx", 1), stride: shifted(blocks[stride], "ctx", 1)}
    return widen(handed, stride // 2)


def earlier_sum(value, axis):
    count = lax.axis_size(axis)
    place = lax.axis_index(axis)
    total = value.astype(F32)
    before = jnp.zeros_like(total)
    bit = 1
    while bit < count:
        slim = total.astype(BF16)
        if 2 * bit < count:
            other = swapped(slim, axis, bit).astype(F32)
        else:
            ahead = [(source, source + bit) for source in range(count - bit)]
            other = lax.ppermute(slim, axis, ahead).astype(F32)
        before = before + jnp.where(place & bit != 0, other, 0.0)
        total = total + other
        bit *= 2
    return before


def fetch(tables, copies, semaphores):
    moves = [
        pltpu.make_async_copy(table, copy, semaphores.at[index])
        for index, (table, copy) in enumerate(zip(tables, copies))
    ]
    for move in moves:
        move.start()
    return moves


def table_scratch(*tables):
    return [pltpu.SMEM(table.shape, table.dtype) for table in tables] + [
        pltpu.SemaphoreType.DMA((len(tables),))
    ]


def clip_span(starts, lens, span, prior):
    place = lax.axis_index("ctx")
    if prior:
        source = jnp.maximum(place - 1, 0)
        shift = span - starts[source]
        length = jnp.where(place > 0, lens[source], 0)
    else:
        shift = -starts[place]
        length = lens[place]
    return shift, length, jnp.maximum(0, -shift), jnp.minimum(span, length - shift)


def clip_rows(rows, count, span):
    me = lax.axis_index("head")
    slot = lax.broadcasted_iota(jnp.int32, (1, span), 1)
    row = slot
    for key in range(count):
        inside = (slot >= key * rows) & (slot < (key + 1) * rows)
        row = jnp.where(inside, slot + ((me ^ key) - key) * rows, row)
    return row


def packed_shape(span, inner):
    whole = inner // 256 * 256
    return span + span * (inner - whole) // whole, whole


def pack(value):
    span, inner = value.shape
    whole = inner // 256 * 256
    groups = whole // (inner - whole)
    rows = span // groups
    tail = jnp.concatenate(
        [value[group * rows : (group + 1) * rows, whole:] for group in range(groups)], axis=1
    )
    return jnp.concatenate([value[:, :whole], tail], axis=0)


def unpack_tail(value, span):
    whole = value.shape[1]
    rows = value.shape[0] - span
    width = rows * whole // span
    return jnp.concatenate(
        [value[span:, group * width : (group + 1) * width] for group in range(span // rows)], axis=0
    )


def output_product(parts, weights, span):
    whole = parts[0].shape[1]
    left = jnp.concatenate(
        [part[:span, :] for part in parts] + [unpack_tail(part[...], span) for part in parts], axis=1
    )
    right = jnp.concatenate(
        [weight[:whole, :] for weight in weights] + [weight[whole:, :] for weight in weights], axis=0
    )
    return dot(left, right)


def mix(pieces, weights, size):
    frame = jnp.concatenate([piece[...] for piece in pieces], axis=0)
    inner = weights.shape[0] // 3
    wide = frame.astype(F32)
    scale = lax.rsqrt(jnp.mean(wide * wide, axis=-1, keepdims=True) + EPS)
    full = dot_t(frame, weights[...])
    return (
        (full[:, :inner] * (scale * (size**-0.5 * math.log2(math.e)))).astype(BF16),
        (full[:, inner : 2 * inner] * scale).astype(BF16),
        (full[:, 2 * inner :] * scale).astype(BF16),
    )


def mix_kernel(size, *refs):
    *pieces, weights, queries, keys, values = refs
    queries[...], keys[...], values[...] = mix(pieces, weights, size)


def mix_rows(pieces, weights, heads):
    rows = pieces[0].shape[0] * len(pieces)
    inner = weights.shape[0] // 3
    return pl.pallas_call(
        functools.partial(mix_kernel, inner // heads),
        out_shape=(jax.ShapeDtypeStruct((rows, inner), BF16),) * 3,
        in_specs=[VMEM] * (len(pieces) + 1),
        out_specs=(VMEM,) * 3,
        compiler_params=pltpu.CompilerParams(vmem_limit_bytes=10 * 2**20),
        cost_estimate=pl.CostEstimate(flops=10**9, bytes_accessed=4 * 10**6, transcendentals=0),
        name="prior_mix",
    )(*pieces, weights)


def attend_kernel(prior, count, heads, block, far_starts, far_lens, *refs):
    *refs, starts, lens, semaphores = refs
    moves = fetch((far_starts, far_lens), (starts, lens), semaphores)
    if prior:
        *refs, old, top, bottom, queries, keys, values, context = refs
        *pieces, weights, near_queries, near_keys, near_values = refs
    else:
        *pieces, weights, context, queries, keys, values = refs
    rows, _ = pieces[0].shape
    span = rows * count
    inner = weights.shape[0] // 3
    size = inner // heads
    row = clip_rows(rows, count, span)
    lane = lax.broadcasted_iota(jnp.int32, (1, inner), 1)
    owner = [(lane >= head * size) & (lane < (head + 1) * size) for head in range(heads)]
    groups = {}
    for head in range(heads):
        groups.setdefault(head * size // 128 * 128, []).append(head)

    def fill(first_row):
        queries[first_row:, :], keys[first_row:, :], values[first_row:, :] = mix(pieces, weights, size)

    if prior:
        context[...] = old[...]
        for move in moves:
            move.wait()
        shift, length, first, last = clip_span(starts, lens, span, prior)

        @pl.when(last > first)
        def _():
            held_rows = near_queries.shape[0]
            queries[:held_rows, :] = near_queries[...]
            keys[:held_rows, :] = near_keys[...]
            values[:held_rows, :] = near_values[...]
            fill(held_rows)

    else:
        context[...] = jnp.zeros_like(context)
        fill(0)
        for move in moves:
            move.wait()
        shift, length, first, last = clip_span(starts, lens, span, prior)

    def step(index, _):
        low = pl.multiple_of(index * block, block)
        place = low + lax.broadcasted_iota(jnp.int32, (block, 1), 0)
        live = (place >= first) & (place < last)
        pick = (place + shift == row) & live
        query = dot(jnp.where(pick, 1.0, 0.0).astype(BF16), queries[...])
        total = jnp.zeros((block, inner), F32)
        for base, members in groups.items():
            end = min(inner, base + 256)
            stack = jnp.concatenate(
                [jnp.where(owner[head], query, 0.0)[:, base:end].astype(BF16) for head in members], axis=0
            )
            scores = dot_t(stack, keys[:, base:end])
            scores = jnp.where(row < length, scores, LOW)
            powers = jnp.exp2(scores - jnp.max(scores, axis=-1, keepdims=True))
            mass = jnp.sum(powers, axis=-1, keepdims=True)
            mixed = dot(powers.astype(BF16), values[:, base:end]) / mass
            for place_in, head in enumerate(members):
                part = mixed[place_in * block : (place_in + 1) * block, :]
                sides = [part]
                if base:
                    sides = [jnp.zeros((block, base), F32)] + sides
                if end < inner:
                    sides = sides + [jnp.zeros((block, inner - end), F32)]
                total = jnp.where(owner[head], jnp.concatenate(sides, axis=1), total)
        here = pl.ds(low, block)
        if prior:
            context[here, :] = jnp.where(live, total, context[here, :].astype(F32)).astype(BF16)
        else:
            context[here, :] = total.astype(BF16)
        return 0

    lax.fori_loop(first // block, jnp.where(last > first, (last + block - 1) // block, 0), step, 0)
    if prior:
        top[...] = pack(context[: span // 2, :])
        bottom[...] = pack(context[span // 2 :, :])


def attend(pieces, weights, starts, lens, heads, near_rows=(), old=()):
    rows, _ = pieces[0].shape
    held_rows = near_rows[0].shape[0] if near_rows else 0
    span = rows * len(pieces) + held_rows
    inner = weights.shape[0] // 3
    extra = [*near_rows, *old]
    return pl.pallas_call(
        functools.partial(attend_kernel, len(old) > 0, span // rows, heads, min(BLOCK, span)),
        out_shape=(jax.ShapeDtypeStruct(packed_shape(span // 2, inner), BF16),) * 2
        if old
        else jax.ShapeDtypeStruct((span, inner), BF16),
        in_specs=[HBM, HBM] + [VMEM] * (len(pieces) + 1 + len(extra)),
        out_specs=(VMEM,) * 2 if old else VMEM,
        scratch_shapes=[pltpu.VMEM((span, inner), BF16)] * (3 + len(old)) + table_scratch(starts, lens),
        compiler_params=pltpu.CompilerParams(vmem_limit_bytes=16 * 2**20),
        cost_estimate=pl.CostEstimate(flops=5 * 10**9, bytes_accessed=4 * 10**6, transcendentals=10**6),
        name="attend_prior" if old else "attend_own",
    )(starts, lens, *pieces, weights, *extra)


def warm_kernel(source, target):
    target[...] = source[...]


def warm(weights):
    return pl.pallas_call(
        warm_kernel,
        out_shape=jax.ShapeDtypeStruct(weights.shape, weights.dtype),
        in_specs=[VMEM],
        out_specs=VMEM,
        compiler_params=pltpu.CompilerParams(vmem_limit_bytes=6 * 2**20),
        cost_estimate=pl.CostEstimate(flops=10**9, bytes_accessed=4 * 10**6, transcendentals=0),
        name="warm",
    )(weights)


def arrange_kernel(sizes, far_starts, far_lens, *refs):
    *refs, base, starts, lens, semaphores = refs
    for move in fetch((far_starts, far_lens), (starts, lens), semaphores):
        move.wait()
    lists, at = [], 0
    for size in sizes:
        lists.append(refs[at : at + size])
        at += size
    top, bottom, outs, own, prior = lists
    span = base.shape[0]
    count = lax.axis_size("head")
    row = clip_rows(span // count, count, span)
    place = lax.broadcasted_iota(jnp.int32, (span, 1), 0)
    total = jnp.concatenate([output_product(parts, outs, span // 2) for parts in (top, bottom)], axis=0)
    for pieces, earlier in ((own, False), (prior, True)):
        shift, length, _, _ = clip_span(starts, lens, span, earlier)
        pick = (place + shift == row) & (row < length)
        frame = jnp.concatenate([piece[...] for piece in pieces], axis=0)
        total = total + dot(jnp.where(pick, 1.0, 0.0).astype(BF16), frame)
    base[...] = total


def arrange(own, prior, halves, outs, starts, lens):
    span = sum(piece.shape[0] for piece in own)
    lists = (*halves, outs, own, prior)
    return pl.pallas_call(
        functools.partial(arrange_kernel, tuple(map(len, lists))),
        out_shape=jax.ShapeDtypeStruct((span, own[0].shape[1]), F32),
        in_specs=[HBM, HBM] + [VMEM] * sum(map(len, lists)),
        out_specs=VMEM,
        scratch_shapes=table_scratch(starts, lens),
        compiler_params=pltpu.CompilerParams(vmem_limit_bytes=16 * 2**20),
        cost_estimate=pl.CostEstimate(flops=2 * 10**9, bytes_accessed=3 * 10**6, transcendentals=0),
        name="arrange",
    )(starts, lens, *[piece for pieces in lists for piece in pieces])


def project_kernel(low, span, far_starts, far_lens, *refs):
    *refs, starts, lens, semaphores = refs
    moves = fetch((far_starts, far_lens), (starts, lens), semaphores)
    base, projector, text, *pieces, result = refs
    parts, weights = pieces[: len(pieces) // 2], pieces[len(pieces) // 2 :]
    rows = result.shape[0]
    here = slice(low, low + rows)
    whole = parts[0].shape[1]
    left = jnp.concatenate(
        [part[:rows, :] for part in parts] + [unpack_tail(part[...], rows) for part in parts], axis=1
    )
    right = jnp.concatenate(
        [weight[:whole, :] for weight in weights] + [weight[whole:, :] for weight in weights], axis=0
    )
    resid = base[here, :] + dot(left, right)
    scale = lax.rsqrt(jnp.mean(resid * resid, axis=-1, keepdims=True) + EPS)
    visual = dot((resid * scale).astype(BF16), projector[...]).astype(BF16)
    for move in moves:
        move.wait()
    _, _, own_first, own_last = clip_span(starts, lens, span, False)
    _, _, prior_first, prior_last = clip_span(starts, lens, span, True)
    place = low + lax.broadcasted_iota(jnp.int32, (rows, 1), 0)
    live = ((place >= own_first) & (place < own_last)) | (
        (place >= prior_first) & (place < prior_last)
    )
    result[...] = jnp.where(live, visual, text[here, :])


def project(low, rows, base, parts, outs, projector, text, starts, lens):
    span, columns = text.shape
    return pl.pallas_call(
        functools.partial(project_kernel, low, span),
        out_shape=jax.ShapeDtypeStruct((rows, columns), BF16),
        in_specs=[HBM, HBM] + [VMEM] * (3 + 2 * len(parts)),
        out_specs=VMEM,
        scratch_shapes=table_scratch(starts, lens),
        compiler_params=pltpu.CompilerParams(vmem_limit_bytes=12 * 2**20),
        cost_estimate=pl.CostEstimate(flops=10**9, bytes_accessed=2 * 10**6, transcendentals=0),
    )(starts, lens, base, projector, text, *parts, *outs)


def held(weights, part, key, depth):
    start = pl.multiple_of((lax.axis_index("head") ^ key) * depth, depth)
    return weights[part, pl.ds(start, depth), :]


def near_kernel(keys, weights, *refs):
    count = len(keys)
    pieces = refs[:count]
    query_sum, pair_sum, squares = refs[count:]
    norm = 0.0
    for piece in pieces:
        wide = piece[...].astype(F32)
        norm = norm + jnp.sum(wide * wide, axis=-1, keepdims=True)
    squares[...] = jnp.broadcast_to(norm, squares.shape)
    for part in range(3):
        total = 0.0
        for index in range(count):
            total = total + dot(pieces[index][...], held(weights, part, keys[index], pieces[index].shape[1]))
        if part == 0:
            query_sum[...] = total
        else:
            pair_sum[part - 1] = total


def near(pieces, keys, weights):
    span, _ = pieces[0].shape
    columns = weights.shape[2]
    return pl.pallas_call(
        functools.partial(near_kernel, keys),
        out_shape=(
            jax.ShapeDtypeStruct((span, columns), F32),
            jax.ShapeDtypeStruct((2, span, columns), F32),
            jax.ShapeDtypeStruct((span, HD), F32),
        ),
        in_specs=[VMEM] * (1 + len(pieces)),
        out_specs=(VMEM, VMEM, VMEM),
        compiler_params=pltpu.CompilerParams(vmem_limit_bytes=12 * 2**20),
        cost_estimate=pl.CostEstimate(flops=3 * 10**9, bytes_accessed=7 * 10**6, transcendentals=0),
    )(weights, *pieces)


def pair_kernel(keys, total_depth, weights, pair_sum, squares, *refs):
    count = len(keys)
    pieces = refs[:count]
    *olds, key_out, value_out, delta, scale_out = refs[count:]
    norm = squares[:, :1]
    for piece in pieces:
        wide = piece[...].astype(F32)
        norm = norm + jnp.sum(wide * wide, axis=-1, keepdims=True)
    scale = lax.rsqrt(norm * (1.0 / total_depth) + EPS)
    scale_out[...] = jnp.broadcast_to(scale, scale_out.shape)
    for part, out in ((0, key_out), (1, value_out)):
        total = pair_sum[part]
        for index in range(count):
            total = total + dot(pieces[index][...], held(weights, part + 1, keys[index], pieces[index].shape[1]))
        out[...] = (total * scale).astype(BF16)
    for head in range(delta.shape[0]):
        lanes = slice(head * HD, (head + 1) * HD)
        product = lax.dot_general(
            key_out[:, lanes], value_out[:, lanes], (((0,), (0,)), ((), ())), preferred_element_type=F32
        )
        if olds:
            product = product + olds[0][head]
        delta[head] = product.astype(delta.dtype)


def pair(kind, pieces, keys, weights, pair_sum, squares, olds):
    span, _ = pieces[0].shape
    columns = weights.shape[2]
    return pl.pallas_call(
        functools.partial(pair_kernel, keys, weights.shape[1]),
        out_shape=(
            jax.ShapeDtypeStruct((span, columns), BF16),
            jax.ShapeDtypeStruct((span, columns), BF16),
            jax.ShapeDtypeStruct((columns // HD, HD, HD), kind),
            jax.ShapeDtypeStruct((span, HD), F32),
        ),
        in_specs=[VMEM] * (3 + len(pieces) + len(olds)),
        out_specs=(VMEM,) * 4,
        compiler_params=pltpu.CompilerParams(vmem_limit_bytes=12 * 2**20),
        cost_estimate=pl.CostEstimate(flops=3 * 10**9, bytes_accessed=7 * 10**6, transcendentals=0),
    )(weights, pair_sum, squares, *pieces, *olds)


def within_kernel(keys, groups, weights, *refs):
    count = len(keys)
    sizes = (groups, groups, groups, groups, groups * count)
    lists, at = [], 0
    for size in sizes:
        lists.append(refs[at : at + size])
        at += size
    query_sums, scales, key_ins, value_ins, pieces = lists
    query_out, intra, buffers, semaphores = refs[at:]
    depth = pieces[0].shape[1]
    starts = [pl.multiple_of((lax.axis_index("head") ^ key) * depth, depth) for key in keys]
    moves = fetch(
        [weights.at[0, pl.ds(start, depth), :] for start in starts],
        [buffers.at[index] for index in range(count)],
        semaphores,
    )
    for move in moves:
        move.wait()
    low = 0
    for group in range(groups):
        rows = query_sums[group].shape[0]
        here = slice(low, low + rows)
        low += rows
        causal = lax.broadcasted_iota(jnp.int32, (rows, rows), 0) >= lax.broadcasted_iota(
            jnp.int32, (rows, rows), 1
        )
        total = query_sums[group][...]
        for index in range(count):
            total = total + dot(pieces[group * count + index][...], buffers[index])
        query_out[here, :] = (total * scales[group][:, :1]).astype(BF16)
        for head in range(query_out.shape[1] // HD):
            lanes = slice(head * HD, (head + 1) * HD)
            query = query_out[here, lanes]
            corner = dot_t(query, key_ins[group][:, lanes])
            corner = jnp.where(causal, corner, 0.0).astype(BF16)
            total = dot(corner, value_ins[group][:, lanes])
            for earlier in range(group):
                left = dot_t(query, key_ins[earlier][:, lanes]).astype(BF16)
                total = total + dot(left, value_ins[earlier][:, lanes])
            intra[here, lanes] = total


def within(pieces, keys, weights, query_sums, scales, key_ins, value_ins):
    depth = pieces[0].shape[1]
    groups = len(query_sums)
    columns = weights.shape[2]
    span = sum(query_sum.shape[0] for query_sum in query_sums)
    return pl.pallas_call(
        functools.partial(within_kernel, keys, groups),
        out_shape=(
            jax.ShapeDtypeStruct((span, columns), BF16),
            jax.ShapeDtypeStruct((span, columns), F32),
        ),
        in_specs=[HBM] + [VMEM] * (4 * groups + len(pieces)),
        out_specs=(VMEM,) * 2,
        scratch_shapes=[
            pltpu.VMEM((len(keys), depth, columns), BF16),
            pltpu.SemaphoreType.DMA((len(keys),)),
        ],
        compiler_params=pltpu.CompilerParams(vmem_limit_bytes=12 * 2**20),
        cost_estimate=pl.CostEstimate(flops=3 * 10**9, bytes_accessed=5 * 10**6, transcendentals=0),
        name="within",
    )(weights, *query_sums, *scales, *key_ins, *value_ins, *pieces)


def finish_kernel(query, intra, carried, state, gain, out):
    for head in range(state.shape[0]):
        lanes = slice(head * HD, (head + 1) * HD)
        whole = (carried[head] + state[head]).astype(BF16)
        lin = intra[:, lanes] + dot(query[:, lanes], whole)
        scale = lax.rsqrt(jnp.mean(lin * lin, axis=-1, keepdims=True) + EPS)
        out[:, lanes] = (lin * scale * gain[:, lanes]).astype(BF16)


def finish(query, intra, carried, state, gain):
    return pl.pallas_call(
        finish_kernel,
        out_shape=jax.ShapeDtypeStruct(query.shape, BF16),
        in_specs=[VMEM] * 5,
        out_specs=VMEM,
        compiler_params=pltpu.CompilerParams(vmem_limit_bytes=8 * 2**20),
        cost_estimate=pl.CostEstimate(flops=10**8, bytes_accessed=3 * 10**6, transcendentals=0),
        name="finish",
    )(query, intra, carried, state, gain.reshape(1, -1))


def program(
    patches,
    clip_start,
    clip_len,
    text_rows,
    vision_qkv,
    vision_out,
    projector,
    layer_qkv,
    head_gain,
    state_in,
):
    groups = lax.axis_size("head")
    heads = VIT_HEADS // groups
    own = spread(patches)
    prior = spread_prior(own)
    outs = spread(vision_out)
    vision = jnp.transpose(vision_qkv, (1, 2, 0)).reshape(-1, vision_qkv.shape[0])
    layer = jnp.transpose(layer_qkv, (1, 0, 2))
    vision = warm(vision)
    context = attend(own, vision, clip_start, clip_len, heads)
    half = groups // 2
    near_rows = mix_rows(prior[:half], vision, heads)
    halves = attend(prior[half:], vision, clip_start, clip_len, heads, near_rows, [context])
    parts = [spread(piece) for piece in halves]
    near_keys, far_keys = tuple(range(half)), tuple(range(half, groups))
    near_parts = [pieces[:half] for pieces in parts]
    base = arrange(own, prior, near_parts, outs[:half], clip_start, clip_len)
    query_sums, scales, key_rows, value_rows, pieces, old = [], [], [], [], [], []
    low = 0
    for index, share in enumerate(SHARES):
        rows = text_rows.shape[0] // share
        sequence = project(
            low, rows, base, parts[index][half:], outs[half:], projector, text_rows, clip_start, clip_len
        )
        low += rows
        blocks = spread(sequence)
        query_sum, pair_sum, squares = near(blocks[:half], near_keys, layer)
        kind = BF16 if index == len(SHARES) - 1 else F32
        key_row, value_row, delta, scale = pair(kind, blocks[half:], far_keys, layer, pair_sum, squares, old)
        old = [delta]
        query_sums.append(query_sum)
        scales.append(scale)
        key_rows.append(key_row)
        value_rows.append(value_row)
        pieces += blocks[half:]
    carried = earlier_sum(delta, "ctx")
    query, intra = within(pieces, far_keys, layer, query_sums, scales, key_rows, value_rows)
    return finish(query, intra, carried, state_in, head_gain)


def solution(mesh):
    placed = (
        P(("ctx", "head"), None),
        P(),
        P(),
        P("ctx", "head"),
        P(None, None, "head"),
        P("head", None),
        P(None, "head"),
        P(None, None, "head"),
        P("head"),
        P("head", None, None),
    )
    return jax.shard_map(program, mesh=mesh, in_specs=placed, out_specs=P("ctx", "head"), check_vma=False)
```
